256 devices in a mesh: grp: 4 (over y), slab: 64 (over z, x, core).
Axes of the slice: x: 4, y: 4, z: 8, core: 2. Of those that a mesh axis runs over, the one named last changes fastest.
Arguments:
- velocity: float32 [16, 3, 4, 131072], P(None, None, 'grp', 'slab'), may hold values from -6 to 6
- old_basis: bfloat16 [64, 3, 4, 131072], P(None, None, None, 'slab'), may hold values from -6 to 6
- singular_values: float32 [64], replicated, may hold values from 0.7 to 1.4
- thickness: int32 [4, 64], P('grp', 'slab'), may hold values from 1 to 4, as said below
Outputs:
- gram_matrix: float32 [80, 80], replicated
- new_basis: bfloat16 [64, 3, 4, 131072], P(None, None, None, 'slab')
- offsets: int32 [4, 64], P('grp', 'slab')
The draws below stay inside these ranges and needn't reach their ends.
Inputs may be any that keep to these rules, and one draw needn't show every extreme that they name: `thickness`: the entry at row-major position p differs from 1 + (p * 3) // 256 by at most one. The first entry is 1 and the last is 4.
All inputs are finite; a program needn't handle non-finite values.
Results may differ from the reference program's by a relative error of at most 0.0004.
The reference program's roundings to bfloat16 on the way (of `snapshot_rows`, `basis_rows`, `stacked` and `mixing_rows`) count: a program that leaves them out, or rounds other values in their place, can miss the bound.
Values may be sent and summed in bfloat16 or wider, within the bound.
No kernel may reach another device: no remote copies, remote signals or barrier semaphores. Data moves between devices by JAX's collectives and lax.ppermute only.
A program may use at most 64 MiB of HBM per device.

```python
import math
import jax
import jax.numpy as jnp
from jax import lax

RANK = 64
SNAPS = 16
MAXP = 4
PLANE = 512
CELLS = 131072
N_GRP = 4
N_SLAB = 64


def draw_thickness(key, part):
    total_slabs = N_GRP * N_SLAB
    flat_ids = jnp.arange(total_slabs, dtype=jnp.int32)
    ramp = 1 + flat_ids * (MAXP - 1) // total_slabs
    jitter = jax.random.randint(key, (total_slabs,), -1, 2)
    values = jnp.clip(ramp + jitter, 1, MAXP)
    values = jnp.where(flat_ids == 0, 1, values)
    values = jnp.where(flat_ids == total_slabs - 1, MAXP, values)
    return values.reshape(N_GRP, N_SLAB).astype(jnp.int32)


def steps_of(rng, dims, split, smallest, high):
    def one(dim, parts):
        heights = jax.random.uniform(jax.random.fold_in(jax.random.fold_in(rng, 6), dim), (parts,), jnp.float32, smallest / len(split), high / len(split))
        return jnp.repeat(jnp.exp(heights), dims[dim] // parts).reshape((-1,) + (1,) * (len(dims) - dim - 1))

    factor_of = one(*split[0])
    for cut in split[1:]:
        factor_of = factor_of * one(*cut)
    return factor_of


def normal_values(own_key, extent, scale, bound, cuts=(), held_as=jnp.bfloat16):
    entries = jax.random.normal(own_key, extent, jnp.float32) * scale
    if len(cuts) > 0:
        entries = steps_of(own_key, extent, cuts, -0.22, 0.18) * entries
    return jnp.clip(entries, min=-bound, max=bound).astype(held_as)


def setup_inputs(seed: int = 0) -> dict:
    key_list = jax.random.split(jax.random.key(seed), 5)
    velocity = normal_values(key_list[0], (SNAPS, 3, N_GRP, CELLS), 1.0, 6.0, ((2, 4), (3, 64)), jnp.float32)
    old_basis = normal_values(key_list[1], (RANK, 3, N_GRP, CELLS), 1.0, 6.0, ((3, 64),))
    singular_values = jnp.clip(jnp.exp(jax.random.uniform(key_list[2], (RANK,), jnp.float32, math.log(0.7), math.log(1.4))), 0.7, 1.4)
    thickness = draw_thickness(jax.random.fold_in(key_list[4], 71), 0)
    return dict(velocity=velocity, old_basis=old_basis, singular_values=singular_values, thickness=thickness)


def orthonormalize(matrix, rank_count):
    iterate = matrix * (0.5 * rank_count ** 0.5 / jnp.sqrt(jnp.sum(matrix * matrix)))
    for sweep_index in range(4):
        product = jnp.dot(iterate.T, iterate, precision=lax.Precision.HIGHEST)
        iterate = 1.5 * iterate - 0.5 * jnp.dot(iterate, product, precision=lax.Precision.HIGHEST)
    return iterate

def reference(velocity, old_basis, singular_values, thickness):
    capacity = MAXP * PLANE
    cell_ids = jnp.arange(N_SLAB * capacity, dtype=jnp.int32)
    owners = cell_ids // capacity
    plane_ids = cell_ids % capacity // PLANE
    live_masks = plane_ids[None, :] < thickness[:, owners]
    snapshot_rows = jnp.where(live_masks[None, None], velocity.astype(jnp.bfloat16), jnp.zeros((), jnp.bfloat16))
    basis_rows = jnp.where(live_masks[None, None], old_basis, jnp.zeros((), jnp.bfloat16))
    stacked = jnp.concatenate([basis_rows.reshape(RANK, -1), snapshot_rows.reshape(SNAPS, -1)], 0)
    live_total = jnp.sum(thickness).astype(jnp.float32) * PLANE
    scales = jnp.concatenate([singular_values.astype(jnp.float32), jnp.ones((SNAPS,), jnp.float32)])
    raw_gram = lax.dot_general(stacked, stacked, (((1,), (1,)), ((), ())), preferred_element_type=jnp.float32)
    gram_matrix = raw_gram * scales[:, None] * scales[None, :] / (3.0 * live_total)
    mixing = orthonormalize(gram_matrix[:, :RANK], RANK)
    mixing_rows = (mixing * scales[:, None]).T.astype(jnp.bfloat16)
    updated = jnp.dot(mixing_rows, stacked, preferred_element_type=jnp.float32).astype(jnp.bfloat16)
    new_basis = updated.reshape(RANK, 3, N_GRP, N_SLAB * capacity)
    flat_counts = thickness.reshape(-1)
    offsets = (jnp.cumsum(flat_counts) - flat_counts).astype(jnp.int32).reshape(N_GRP, N_SLAB)
    return (gram_matrix, new_basis, offsets)
```

```python
import functools

import jax
import jax.numpy as jnp
from jax import lax
from jax.experimental import pallas as pl
from jax.experimental.pallas import tpu as pltpu
from jax.sharding import Mesh
from jax.sharding import PartitionSpec as P

PLANE = 512
SLAB = ("slab_0", "slab_1", "slab_2")

R = 64
S = 16
N = R + S
G = 4
COLS = 6144
J = 48
PITCH = 192
HIGHEST = lax.Precision.HIGHEST


def vmem(n=1):
    return [pl.BlockSpec(memory_space=pltpu.VMEM) for _ in range(n)]


def smem():
    return pl.BlockSpec(memory_space=pltpu.SMEM)


def snapshots_body(thick_ref, vel_ref, out_ref):
    live_tiles = thick_ref[0, 0] * (PLANE // 128)
    for j in range(J):
        rows = vel_ref[pl.ds(j, S, stride=J), :]
        keep = jnp.where(j % 16 < live_tiles, 1, 0)
        rows = jnp.where(jnp.full(rows.shape, keep, jnp.int32) > 0, rows, 0.0)
        out_ref[:, pl.ds(j * 128, 128)] = rows.astype(jnp.bfloat16)


def snapshots(velocity, thickness):
    return pl.pallas_call(
        snapshots_body,
        out_shape=jax.ShapeDtypeStruct((S, COLS), jnp.bfloat16),
        in_specs=[smem()] + vmem(),
        out_specs=vmem()[0],
        name="snapshots",
    )(thickness, velocity.reshape(S * J, 128))


def gram_body(thick_ref, basis_ref, snap_ref, wide_ref, keep_ref, send_ref, f_ref):
    g = lax.axis_index("grp")
    core = lax.axis_index("slab_2")
    place = ((g * 8 + lax.axis_index("slab_0")) * 4 + lax.axis_index("slab_1")) * 2 + core
    thick = thick_ref[0, 0]

    def widen(r, _):
        f_ref[pl.ds(pl.multiple_of(r * PITCH, 8), PITCH), :] = basis_ref[r].astype(jnp.float32)
        return 0

    lax.fori_loop(0, R, widen, 0)
    for k in range(G):
        for j in range(J):
            rows = f_ref[pl.ds(j * G + k, R, stride=PITCH), :]
            wide_ref[k, :, pl.ds(j * 128, 128)] = rows.astype(jnp.bfloat16)
    own = wide_ref[g]
    cols = lax.broadcasted_iota(jnp.int32, (R, COLS), 1)
    own = jnp.where((cols % 2048) // PLANE < thick, own, jnp.zeros((), jnp.bfloat16))
    stacked = jnp.concatenate([own, snap_ref[...], jnp.zeros((128 - N, COLS), jnp.bfloat16)], 0)
    gram = lax.dot_general(
        stacked, stacked, (((1,), (1,)), ((), ())), preferred_element_type=jnp.float32
    )
    lane = lax.broadcasted_iota(jnp.int32, (16, 128), 1)
    row = lax.broadcasted_iota(jnp.int32, (16, 128), 0)
    thick_block = jnp.where(row * 16 + lane == place, thick.astype(jnp.float32), 0.0)
    upper = jnp.where(lane < 80, gram[0:16], pltpu.roll(gram[32:48], 48, 1))
    last = jnp.where(lane < 112, pltpu.roll(gram[48:64], 32, 1), pltpu.roll(gram[64:80], 48, 1))
    lower = jnp.where(lane < 16, thick_block, jnp.where(lane < 80, gram[16:32], last))
    first = jnp.full((16, 128), core, jnp.int32) == 0
    keep_ref[...] = jnp.where(first, upper, lower)
    send_ref[...] = jnp.where(first, lower, upper)


def gram_partial(thickness, basis, snap):
    half = jax.ShapeDtypeStruct((16, 128), jnp.float32)
    return pl.pallas_call(
        gram_body,
        out_shape=(jax.ShapeDtypeStruct((G, R, COLS), jnp.bfloat16), half, half),
        in_specs=[smem()] + vmem(2),
        out_specs=vmem(3),
        scratch_shapes=[pltpu.VMEM((R * PITCH, 128), jnp.float32)],
        name="gram",
    )(thickness, basis, snap)


def update_body(mine_ref, other_ref, sv_ref, wide_ref, s0, s1, s2, s3, gram_ref, new_ref, off_ref, snap_ref, f_ref, out_ref, sems):
    g = lax.axis_index("grp")
    core = lax.axis_index("slab_2")
    slab = (lax.axis_index("slab_0") * 4 + lax.axis_index("slab_1")) * 2 + core
    place = g * 64 + slab
    for k, ref in enumerate((s0, s1, s2, s3)):
        snap_ref[g ^ k] = ref[...]
    mine, other = mine_ref[...], other_ref[...]
    first = jnp.full((16, 128), core, jnp.int32) == 0
    upper, lower = jnp.where(first, mine, other), jnp.where(first, other, mine)
    lane = lax.broadcasted_iota(jnp.int32, (16, 128), 1)
    row = lax.broadcasted_iota(jnp.int32, (16, 128), 0)
    order = row * 16 + lane
    thick = jnp.where(lane < 16, lower, 0.0)
    before = jnp.sum(jnp.where(order < place, thick, 0.0))
    off_ref[0, 0] = before.astype(jnp.int32)
    live = jnp.sum(thick) * PLANE
    blocks = (
        upper,
        lower,
        pltpu.roll(upper, 128 - 48, 1),
        pltpu.roll(lower, 128 - 32, 1),
        pltpu.roll(lower, 128 - 48, 1),
    )
    diag = [jnp.where((lane >= 16 * i) & (lane < 80), b, 0.0) for i, b in enumerate(blocks)]
    strict = [jnp.where(lane >= 16 * (i + 1), b, 0.0) for i, b in enumerate(diag)]
    pad = [jnp.zeros((48, 128), jnp.float32)]
    raw = jnp.concatenate(diag + pad, 0) + jnp.concatenate(strict + pad, 0).T
    scale_row = jnp.concatenate([sv_ref[...], jnp.ones((1, 128 - R), jnp.float32)], 1)
    scale_cols = jnp.broadcast_to(scale_row, (128, 128))
    scale_rows = scale_cols.T
    full = raw * scale_rows * scale_cols / (3.0 * live)
    gram_ref[...] = full[:N, :N]
    it = full[:R]
    it = it * (0.5 * R**0.5 / jnp.sqrt(jnp.sum(it * it)))
    for _ in range(4):
        prod = lax.dot_general(it, it, (((1,), (1,)), ((), ())), precision=HIGHEST)
        it = 1.5 * it - 0.5 * jnp.dot(prod, it, precision=HIGHEST)
    mix = (it * scale_cols[:R])[:, :N].astype(jnp.bfloat16)
    slab_thick = [
        jnp.sum(jnp.where(order == k * 64 + slab, thick, 0.0)).astype(jnp.int32) for k in range(G)
    ]
    tile_cols = lax.broadcasted_iota(jnp.int32, (R, 2048), 1) // PLANE
    copies = []
    for c in range(3):
        for k in range(G):
            cols = pl.ds(c * 2048, 2048)
            stacked = jnp.concatenate([wide_ref[k, :, cols], snap_ref[k, :, cols]], 0)
            res = jnp.dot(mix, stacked, preferred_element_type=jnp.float32)
            res = jnp.where(tile_cols < slab_thick[k], res, 0.0)
            for t in range(16):
                f_ref[pl.ds((c * 16 + t) * G + k, R, stride=PITCH), :] = res[:, t * 128 : (t + 1) * 128]

        def narrow(r, _):
            at = pl.multiple_of(r * PITCH + c * 64, 8)
            out_ref[r, pl.ds(c * 64, 64), :] = f_ref[pl.ds(at, 64), :].astype(jnp.bfloat16)
            return 0

        lax.fori_loop(0, R, narrow, 0)
        part = pl.ds(c * 64, 64)
        copy = pltpu.make_async_copy(out_ref.at[:, part], new_ref.at[:, part], sems.at[c])
        copy.start()
        copies.append(copy)
    for copy in copies:
        copy.wait()


def update(mine, other, sv, wide, snaps):
    return pl.pallas_call(
        update_body,
        out_shape=(
            jax.ShapeDtypeStruct((N, N), jnp.float32),
            jax.ShapeDtypeStruct((R, PITCH, 128), jnp.bfloat16),
            jax.ShapeDtypeStruct((1, 1), jnp.int32),
        ),
        in_specs=vmem(8),
        out_specs=(vmem()[0], pl.BlockSpec(memory_space=pl.ANY), smem()),
        scratch_shapes=[
            pltpu.VMEM((G, S, COLS), jnp.bfloat16),
            pltpu.VMEM((R * PITCH, 128), jnp.float32),
            pltpu.VMEM((R, PITCH, 128), jnp.bfloat16),
            pltpu.SemaphoreType.DMA((3,)),
        ],
        name="update",
    )(mine, other, sv.reshape(1, R), wide, *snaps)


def from_everyone(value, axis):
    size = lax.axis_size(axis)
    return lax.all_to_all(
        jnp.broadcast_to(value[None], (size, *value.shape)), axis, 0, 0, tiled=True
    )


def per_device(velocity, old_basis, singular_values, thickness):
    snap = snapshots(velocity, thickness)
    snaps = [snap] + [lax.ppermute(snap, "grp", [(i, i ^ k) for i in range(G)]) for k in (1, 2, 3)]
    basis = old_basis.reshape(R, 3, G, 16, 128).transpose(0, 1, 3, 2, 4).reshape(R, PITCH, 128)
    wide, keep, send = gram_partial(thickness, basis, snap)
    swap = [(0, 1), (1, 0)]
    half = keep + lax.ppermute(send, "slab_2", swap)
    half = jnp.sum(from_everyone(half, "slab_0"), axis=0)
    half = jnp.sum(from_everyone(half, ("grp", "slab_1")), axis=0)
    other = lax.ppermute(half, "slab_2", swap)
    gram_matrix, new, offsets = update(half, other, singular_values, wide, snaps)
    new_basis = new.reshape(R, 3, 16, G, 128).transpose(0, 1, 3, 2, 4).reshape(R, 3, G, 2048)
    return (gram_matrix, new_basis, offsets)


def solution(mesh):
    split = Mesh(
        mesh.devices.reshape(mesh.shape["grp"], 8, 4, 2), ("grp", "slab_0", "slab_1", "slab_2")
    )
    in_specs = (P(None, None, "grp", SLAB), P(None, None, None, SLAB), P(), P("grp", SLAB))
    out_specs = (P(), P(None, None, None, SLAB), P("grp", SLAB))
    return jax.shard_map(
        per_device, mesh=split, in_specs=in_specs, out_specs=out_specs, check_vma=False
    )
```

```python
import jax
import jax.numpy as jnp
from jax import lax
from jax.experimental import pallas as pl
from jax.experimental.pallas import tpu as pltpu
from jax.sharding import Mesh
from jax.sharding import PartitionSpec as P


PLANE = 512
SLAB = ("slab_0", "slab_1", "slab_2")

R = 64
S = 16
N = R + S
G = 4
COLS = 6144
J = 48
ROWS = 192
PITCH = ROWS + 1
WIDE = (R + 1) * PITCH + 7
HIGHEST = lax.Precision.HIGHEST
MIB = 2**20


def vmem(n=1):
    return [pl.BlockSpec(memory_space=pltpu.VMEM) for _ in range(n)]


def smem():
    return pl.BlockSpec(memory_space=pltpu.SMEM)


def hbm(n=1):
    return [pl.BlockSpec(memory_space=pltpu.HBM) for _ in range(n)]


def near(x):
    return pltpu.with_memory_space_constraint(x, pltpu.VMEM)


def far(x):
    return pltpu.with_memory_space_constraint(x, pltpu.HBM)


def live_tile(t, thick, rows):
    return jnp.full((rows, 128), jnp.where(t // 4 < thick, 1, 0), jnp.int32) > 0


def snapshots_body(thick_ref, vel_hbm, snap_ref, vel_ref, sem):
    get = pltpu.make_async_copy(vel_hbm, vel_ref, sem)
    get.start()
    get.wait()
    thick = thick_ref[0, 0]
    for j in range(J):
        rows = vel_ref[pl.ds(j, S, stride=J), :]
        rows = jnp.where(live_tile(j % 16, thick, S), rows, 0.0)
        snap_ref[:, pl.ds(j * 128, 128)] = rows.astype(jnp.bfloat16)


def snapshots(thickness, velocity):
    return pl.pallas_call(
        snapshots_body,
        out_shape=pltpu.VMEM((S, COLS), jnp.bfloat16),
        in_specs=[smem()] + hbm(),
        out_specs=vmem()[0],
        scratch_shapes=[pltpu.VMEM((S * J, 128), jnp.float32), pltpu.SemaphoreType.DMA(())],
        compiler_params=pltpu.CompilerParams(vmem_limit_bytes=2 * MIB),
        cost_estimate=pl.CostEstimate(flops=2 * 10**9, transcendentals=0, bytes_accessed=10**6),
        name="snapshots",
    )(thickness, far(velocity.reshape(S * J, 128)))


def gram_body(thick_ref, basis_ref, snap_ref, wide_ref, keep_ref, send_ref, stack_ref):
    g = lax.axis_index("grp")
    core = lax.axis_index("slab_2")
    place = ((g * 8 + lax.axis_index("slab_0")) * 4 + lax.axis_index("slab_1")) * 2 + core
    thick = thick_ref[0, 0]

    def widen(r, _):
        wide_ref[pl.ds(r * PITCH, ROWS), :] = basis_ref[r].astype(jnp.float32)
        return 0

    lax.fori_loop(0, R, widen, 0, unroll=4)
    for j in range(J):
        rows = wide_ref[pl.ds(j * G + g, R, stride=PITCH), :]
        rows = jnp.where(live_tile(j % 16, thick, R), rows, 0.0)
        stack_ref[0:R, pl.ds(j * 128, 128)] = rows.astype(jnp.bfloat16)
    stack_ref[R:N, :] = snap_ref[...]
    stack_ref[N:, :] = jnp.zeros((128 - N, COLS), jnp.bfloat16)
    stacked = stack_ref[...]
    gram = lax.dot_general(
        stacked, stacked, (((1,), (1,)), ((), ())), preferred_element_type=jnp.float32
    )
    lane = lax.broadcasted_iota(jnp.int32, (16, 128), 1)
    row = lax.broadcasted_iota(jnp.int32, (16, 128), 0)
    thick_block = jnp.where(row * 16 + lane == place, thick.astype(jnp.float32), 0.0)
    upper = jnp.where(lane < 80, gram[0:16], pltpu.roll(gram[32:48], 48, 1))
    last = jnp.where(lane < 112, pltpu.roll(gram[48:64], 32, 1), pltpu.roll(gram[64:80], 48, 1))
    lower = jnp.where(lane < 16, thick_block, jnp.where(lane < 80, gram[16:32], last))
    first = jnp.full((16, 128), core, jnp.int32) == 0
    keep_ref[0] = jnp.where(first, upper, lower)
    send_ref[0] = jnp.where(first, lower, upper)


def gram_partial(thickness, basis, snap):
    half = pltpu.VMEM((1, 16, 128), jnp.float32)
    return pl.pallas_call(
        gram_body,
        out_shape=(pltpu.VMEM((WIDE, 128), jnp.float32), half, half),
        in_specs=[smem()] + vmem(2),
        out_specs=vmem(3),
        scratch_shapes=[pltpu.VMEM((128, COLS), jnp.bfloat16)],
        compiler_params=pltpu.CompilerParams(vmem_limit_bytes=8 * MIB),
        cost_estimate=pl.CostEstimate(flops=10**9, transcendentals=0, bytes_accessed=10**7),
        name="gram",
    )(thickness, near(basis), near(snap))


def combine_body(*refs):
    *ins, out_ref = refs
    pieces = [ref[i] for ref in ins for i in range(ref.shape[0])]
    while len(pieces) > 1:
        pieces = [sum(pieces[i : i + 2]) for i in range(0, len(pieces), 2)]
    for i in range(out_ref.shape[0]):
        out_ref[i] = pieces[0]


def combine(arrays, copies):
    return pl.pallas_call(
        combine_body,
        out_shape=pltpu.VMEM((copies, 16, 128), jnp.float32),
        in_specs=vmem(len(arrays)),
        out_specs=vmem()[0],
        compiler_params=pltpu.CompilerParams(vmem_limit_bytes=MIB),
        name="combine",
    )(*(near(a) for a in arrays))


def update_body(mine_ref, other_ref, sv_ref, s0, s1, s2, s3, wide_ref, gram_ref, new_ref, off_ref, snap_ref, f_ref, out_ref, sems):
    g = lax.axis_index("grp")
    core = lax.axis_index("slab_2")
    slab = (lax.axis_index("slab_0") * 4 + lax.axis_index("slab_1")) * 2 + core
    place = g * 64 + slab
    for k, ref in enumerate((s0, s1, s2, s3)):
        snap_ref[g ^ k] = ref[...]
    mine, other = mine_ref[0], other_ref[0]
    first = jnp.full((16, 128), core, jnp.int32) == 0
    upper, lower = jnp.where(first, mine, other), jnp.where(first, other, mine)
    lane = lax.broadcasted_iota(jnp.int32, (16, 128), 1)
    row = lax.broadcasted_iota(jnp.int32, (16, 128), 0)
    order = row * 16 + lane
    thick = jnp.where(lane < 16, lower, 0.0)
    before = jnp.sum(jnp.where(order < place, thick, 0.0))
    off_ref[0, 0] = before.astype(jnp.int32)
    live = jnp.sum(thick) * PLANE
    blocks = (
        upper,
        lower,
        pltpu.roll(upper, 128 - 48, 1),
        pltpu.roll(lower, 128 - 32, 1),
        pltpu.roll(lower, 128 - 48, 1),
    )
    diag = [jnp.where((lane >= 16 * i) & (lane < 80), b, 0.0) for i, b in enumerate(blocks)]
    strict = [jnp.where(lane >= 16 * (i + 1), b, 0.0) for i, b in enumerate(diag)]
    pad = [jnp.zeros((48, 128), jnp.float32)]
    raw = jnp.concatenate(diag + pad, 0) + jnp.concatenate(strict + pad, 0).T
    scale_row = jnp.concatenate([sv_ref[...], jnp.ones((1, 128 - R), jnp.float32)], 1)
    scale_cols = jnp.broadcast_to(scale_row, (128, 128))
    scale_rows = scale_cols.T
    full = raw * scale_rows * scale_cols / (3.0 * live)
    gram_ref[...] = full[:N, :N]
    it = full[:R]
    it = it * (0.5 * R**0.5 / jnp.sqrt(jnp.sum(it * it)))
    for _ in range(4):
        prod = lax.dot_general(it, it, (((1,), (1,)), ((), ())), precision=HIGHEST)
        it = 1.5 * it - 0.5 * jnp.dot(prod, it, precision=HIGHEST)
    mix = (it * scale_cols[:R])[:, :N].astype(jnp.bfloat16)
    slab_thick = [
        jnp.sum(jnp.where(order == k * 64 + slab, thick, 0.0)).astype(jnp.int32) for k in range(G)
    ]
    copies = []
    for c in range(3):
        for k in range(G):
            tiles = range(c * 16, c * 16 + 16)
            parts = [wide_ref[pl.ds(j * G + k, R, stride=PITCH), :].astype(jnp.bfloat16) for j in tiles]
            snap = snap_ref[k, :, pl.ds(c * 2048, 2048)]
            stacked = jnp.concatenate([jnp.concatenate(parts, 1), snap], 0)
            res = jnp.dot(mix, stacked, preferred_element_type=jnp.float32)
            for t, j in enumerate(tiles):
                part = jnp.where(live_tile(t, slab_thick[k], R), res[:, t * 128 : (t + 1) * 128], 0.0)
                f_ref[pl.ds(j * G + k, R, stride=PITCH), :] = part

        def narrow(r, _):
            part = f_ref[pl.ds(r * PITCH + c * 64, 64), :]
            out_ref[r, pl.ds(c * 64, 64), :] = part.astype(jnp.bfloat16)
            return 0

        lax.fori_loop(0, R, narrow, 0, unroll=4)
        part = pl.ds(c * 64, 64)
        copy = pltpu.make_async_copy(out_ref.at[:, part], new_ref.at[:, part], sems.at[c])
        copy.start()
        copies.append(copy)
    for copy in copies:
        copy.wait()


def update(mine, other, sv, wide, snaps):
    return pl.pallas_call(
        update_body,
        out_shape=(
            jax.ShapeDtypeStruct((N, N), jnp.float32),
            jax.ShapeDtypeStruct((R, ROWS, 128), jnp.bfloat16),
            jax.ShapeDtypeStruct((1, 1), jnp.int32),
        ),
        in_specs=vmem(8),
        out_specs=(vmem()[0], pl.BlockSpec(memory_space=pl.ANY), smem()),
        scratch_shapes=[
            pltpu.VMEM((G, S, COLS), jnp.bfloat16),
            pltpu.VMEM((WIDE, 128), jnp.float32),
            pltpu.VMEM((R, ROWS, 128), jnp.bfloat16),
            pltpu.SemaphoreType.DMA((3,)),
        ],
        compiler_params=pltpu.CompilerParams(vmem_limit_bytes=20 * MIB),
        name="update",
    )(near(mine), near(other), near(sv.reshape(1, R)), *(near(s) for s in snaps), near(wide))


def from_region(snap, k):
    return lax.ppermute(snap, "grp", [(i, i ^ k) for i in range(G)])


def per_device(velocity, old_basis, singular_values, thickness):
    basis = old_basis.reshape(R, 3, G, 16, 128).transpose(0, 1, 3, 2, 4).reshape(R, ROWS, 128)
    snap = snapshots(thickness, velocity)
    snaps = [snap] + [from_region(snap, k) for k in (1, 2, 3)]
    wide, keep, send = gram_partial(thickness, basis, snap)
    swap = [(0, 1), (1, 0)]
    got = lax.ppermute(send, "slab_2", swap)
    for axis, size in (("slab_0", 8), (("grp", "slab_1"), 16)):
        spread = combine((keep, got) if size == 8 else (got,), size)
        got = lax.all_to_all(spread, axis, 0, 0, tiled=True)
    half = combine((got,), 1)
    other = lax.ppermute(half, "slab_2", swap)
    gram_matrix, new, offsets = update(half, other, singular_values, wide, snaps)
    new_basis = new.reshape(R, 3, 16, G, 128).transpose(0, 1, 3, 2, 4).reshape(R, 3, G, 2048)
    return (gram_matrix, new_basis, offsets)


def solution(mesh):
    split = Mesh(
        mesh.devices.reshape(mesh.shape["grp"], 8, 4, 2), ("grp", "slab_0", "slab_1", "slab_2")
    )
    in_specs = (P(None, None, "grp", SLAB), P(None, None, None, SLAB), P(), P("grp", SLAB))
    out_specs = (P(), P(None, None, None, SLAB), P("grp", SLAB))
    return jax.shard_map(
        per_device, mesh=split, in_specs=in_specs, out_specs=out_specs, check_vma=False
    )
```

```python
import jax
import jax.numpy as jnp
from jax import lax
from jax.experimental import pallas as pl
from jax.experimental.pallas import tpu as pltpu
from jax.sharding import Mesh
from jax.sharding import PartitionSpec as P


PLANE = 512
SLAB = ("slab_0", "slab_1", "slab_2")

R = 64
S = 16
N = R + S
G = 4
COLS = 6144
J = 48
ROWS = 192
VPITCH = J + 8
PITCH = ROWS + 1
WIDE = (R + 1) * PITCH + 7
HIGHEST = lax.Precision.HIGHEST
MIB = 2**20


def vmem(n=1):
    return [pl.BlockSpec(memory_space=pltpu.VMEM) for _ in range(n)]


def smem():
    return pl.BlockSpec(memory_space=pltpu.SMEM)


def hbm(n=1):
    return [pl.BlockSpec(memory_space=pltpu.HBM) for _ in range(n)]


def near(x):
    return pltpu.with_memory_space_constraint(x, pltpu.VMEM)


def far(x):
    return pltpu.with_memory_space_constraint(x, pltpu.HBM)


def live_tile(t, thick, rows):
    return jnp.full((rows, 128), jnp.where(t // 4 < thick, 1, 0), jnp.int32) > 0


def snapshots_body(vel_hbm, snap_ref, vel_ref, sem):
    get = pltpu.make_async_copy(vel_hbm, vel_ref.at[:, 0:J], sem)
    get.start()
    get.wait()
    rows_ref = vel_ref.reshape(S * VPITCH, 128)
    for j in range(J):
        rows = rows_ref[pl.ds(j, S, stride=VPITCH), :]
        snap_ref[:, pl.ds(j * 128, 128)] = rows.astype(jnp.bfloat16)


def snapshots(velocity):
    return pl.pallas_call(
        snapshots_body,
        out_shape=pltpu.VMEM((S, COLS), jnp.bfloat16),
        in_specs=hbm(),
        out_specs=vmem()[0],
        scratch_shapes=[pltpu.VMEM((S, VPITCH, 128), jnp.float32), pltpu.SemaphoreType.DMA(())],
        compiler_params=pltpu.CompilerParams(vmem_limit_bytes=2 * MIB),
        cost_estimate=pl.CostEstimate(flops=2 * 10**9, transcendentals=0, bytes_accessed=10**6),
        name="snapshots",
    )(far(velocity.reshape(S, J, 128)))


def gram_body(thick_ref, basis_ref, snap_ref, wide_ref, part_ref, stack_ref):
    g = lax.axis_index("grp")
    core = lax.axis_index("slab_2")
    place = ((g * 8 + lax.axis_index("slab_0")) * 4 + lax.axis_index("slab_1")) * 2 + core
    thick = thick_ref[0, 0]

    def widen(r, _):
        wide_ref[pl.ds(r * PITCH, ROWS), :] = basis_ref[r].astype(jnp.float32)
        return 0

    lax.fori_loop(0, R, widen, 0, unroll=4)
    for j in range(J):
        rows = wide_ref[pl.ds(j * G + g, R, stride=PITCH), :]
        rows = jnp.where(live_tile(j % 16, thick, R), rows, 0.0)
        stack_ref[0:R, pl.ds(j * 128, 128)] = rows.astype(jnp.bfloat16)
        stack_ref[R:N, pl.ds(j * 128, 128)] = jnp.where(
            live_tile(j % 16, thick, S), snap_ref[:, pl.ds(j * 128, 128)], jnp.zeros((), jnp.bfloat16)
        )
    stack_ref[N:, :] = jnp.zeros((128 - N, COLS), jnp.bfloat16)
    stacked = stack_ref[...]
    gram = lax.dot_general(
        stacked, stacked, (((1,), (1,)), ((), ())), preferred_element_type=jnp.float32
    )
    lane = lax.broadcasted_iota(jnp.int32, (16, 128), 1)
    row = lax.broadcasted_iota(jnp.int32, (16, 128), 0)
    thick_block = jnp.where(row * 16 + lane == place, thick.astype(jnp.float32), 0.0)
    upper = jnp.where(lane < 80, gram[0:16], pltpu.roll(gram[32:48], 48, 1))
    last = jnp.where(lane < 112, pltpu.roll(gram[48:64], 32, 1), pltpu.roll(gram[64:80], 48, 1))
    lower = jnp.where(lane < 16, thick_block, jnp.where(lane < 80, gram[16:32], last))
    part_ref[0, 0:16] = upper
    part_ref[0, 16:32] = lower


def gram_partial(thickness, basis, snap):
    return pl.pallas_call(
        gram_body,
        out_shape=(pltpu.VMEM((WIDE, 128), jnp.float32), pltpu.VMEM((1, 32, 128), jnp.float32)),
        in_specs=[smem()] + vmem(2),
        out_specs=vmem(2),
        scratch_shapes=[pltpu.VMEM((128, COLS), jnp.bfloat16)],
        compiler_params=pltpu.CompilerParams(vmem_limit_bytes=8 * MIB),
        cost_estimate=pl.CostEstimate(flops=10**9, transcendentals=0, bytes_accessed=10**7),
        name="gram",
    )(thickness, near(basis), near(snap))


def tree_sum(pieces):
    while len(pieces) > 1:
        pieces = [sum(pieces[i + 1 : i + 2], pieces[i]) for i in range(0, len(pieces), 2)]
    return pieces[0]


def combine_body(*refs):
    *ins, out_ref = refs
    pieces = [ref[i] for ref in ins for i in range(ref.shape[0])]
    total = tree_sum(pieces)
    for i in range(out_ref.shape[0]):
        out_ref[i] = total


def combine(arrays, copies):
    return pl.pallas_call(
        combine_body,
        out_shape=pltpu.VMEM((copies, 32, 128), jnp.float32),
        in_specs=vmem(len(arrays)),
        out_specs=vmem()[0],
        compiler_params=pltpu.CompilerParams(vmem_limit_bytes=MIB),
        name="combine",
    )(*(near(a) for a in arrays))


def update_body(total_ref, sv_ref, s0, s1, s2, s3, wide_ref, gram_ref, new_ref, off_ref, snap_ref, f_ref, out_ref, sems):
    g = lax.axis_index("grp")
    core = lax.axis_index("slab_2")
    slab = (lax.axis_index("slab_0") * 4 + lax.axis_index("slab_1")) * 2 + core
    place = g * 64 + slab
    for k, ref in enumerate((s0, s1, s2, s3)):
        snap_ref[g ^ k] = ref[...]
    upper, lower = total_ref[0, 0:16], total_ref[0, 16:32]
    lane = lax.broadcasted_iota(jnp.int32, (16, 128), 1)
    row = lax.broadcasted_iota(jnp.int32, (16, 128), 0)
    order = row * 16 + lane
    thick = jnp.where(lane < 16, lower, 0.0)
    before = jnp.sum(jnp.where(order < place, thick, 0.0))
    off_ref[0, 0] = before.astype(jnp.int32)
    live = jnp.sum(thick) * PLANE
    blocks = (
        upper,
        lower,
        pltpu.roll(upper, 128 - 48, 1),
        pltpu.roll(lower, 128 - 32, 1),
        pltpu.roll(lower, 128 - 48, 1),
    )
    diag = [jnp.where((lane >= 16 * i) & (lane < 80), b, 0.0) for i, b in enumerate(blocks)]
    strict = [jnp.where(lane >= 16 * (i + 1), b, 0.0) for i, b in enumerate(diag)]
    pad = [jnp.zeros((48, 128), jnp.float32)]
    raw = jnp.concatenate(diag + pad, 0) + jnp.concatenate(strict + pad, 0).T
    scale_row = jnp.concatenate([sv_ref[...], jnp.ones((1, 128 - R), jnp.float32)], 1)
    scale_cols = jnp.broadcast_to(scale_row, (128, 128))
    scale_rows = scale_cols.T
    full = raw * scale_rows * scale_cols / (3.0 * live)
    gram_ref[...] = full[:N, :N]
    it = full[:R]
    it = it * (0.5 * R**0.5 / jnp.sqrt(jnp.sum(it * it)))
    for _ in range(4):
        prod = lax.dot_general(it, it, (((1,), (1,)), ((), ())), precision=HIGHEST)
        it = 1.5 * it - 0.5 * jnp.dot(prod, it, precision=HIGHEST)
    mix = (it * scale_cols[:R])[:, :N].astype(jnp.bfloat16)
    slab_thick = [
        jnp.sum(jnp.where(order == k * 64 + slab, thick, 0.0)).astype(jnp.int32) for k in range(G)
    ]
    copies = []
    for c in range(3):
        for k in range(G):
            tiles = range(c * 16, c * 16 + 16)
            parts = [wide_ref[pl.ds(j * G + k, R, stride=PITCH), :].astype(jnp.bfloat16) for j in tiles]
            snap = snap_ref[k, :, pl.ds(c * 2048, 2048)]
            stacked = jnp.concatenate([jnp.concatenate(parts, 1), snap], 0)
            res = jnp.dot(mix, stacked, preferred_element_type=jnp.float32)
            for t, j in enumerate(tiles):
                part = jnp.where(live_tile(t, slab_thick[k], R), res[:, t * 128 : (t + 1) * 128], 0.0)
                f_ref[pl.ds(j * G + k, R, stride=PITCH), :] = part

        def narrow(r, _):
            part = f_ref[pl.ds(r * PITCH + c * 64, 64), :]
            out_ref[r, pl.ds(c * 64, 64), :] = part.astype(jnp.bfloat16)
            return 0

        lax.fori_loop(0, R, narrow, 0, unroll=4)
        part = pl.ds(c * 64, 64)
        copy = pltpu.make_async_copy(out_ref.at[:, part], new_ref.at[:, part], sems.at[c])
        copy.start()
        copies.append(copy)
    for copy in copies:
        copy.wait()


def update(total, sv, wide, snaps):
    return pl.pallas_call(
        update_body,
        out_shape=(
            jax.ShapeDtypeStruct((N, N), jnp.float32),
            jax.ShapeDtypeStruct((R, ROWS, 128), jnp.bfloat16),
            jax.ShapeDtypeStruct((1, 1), jnp.int32),
        ),
        in_specs=vmem(7),
        out_specs=(vmem()[0], pl.BlockSpec(memory_space=pl.ANY), smem()),
        scratch_shapes=[
            pltpu.VMEM((G, S, COLS), jnp.bfloat16),
            pltpu.VMEM((WIDE, 128), jnp.float32),
            pltpu.VMEM((R, ROWS, 128), jnp.bfloat16),
            pltpu.SemaphoreType.DMA((3,)),
        ],
        compiler_params=pltpu.CompilerParams(vmem_limit_bytes=20 * MIB),
        name="update",
    )(near(total), near(sv.reshape(1, R)), *(near(s) for s in snaps), near(wide))


def from_region(snap, k):
    return lax.ppermute(snap, "grp", [(i, i ^ k) for i in range(G)])


def per_device(velocity, old_basis, singular_values, thickness):
    basis = old_basis.reshape(R, 3, G, 16, 128).transpose(0, 1, 3, 2, 4).reshape(R, ROWS, 128)
    snap = snapshots(velocity)
    thickness = lax.optimization_barrier((thickness, snap))[0]
    snaps = [snap] + [from_region(snap, k) for k in (1, 2, 3)]
    wide, part = gram_partial(thickness, basis, snap)
    got = lax.ppermute(part, "slab_2", [(0, 1), (1, 0)])
    for axis, size in (("slab_0", 8), (("grp", "slab_1"), 16)):
        spread = combine((part, got) if size == 8 else (got,), size)
        got = lax.all_to_all(spread, axis, 0, 0, tiled=True)
    total = combine((got,), 1)
    gram_matrix, new, offsets = update(total, singular_values, wide, snaps)
    new_basis = new.reshape(R, 3, 16, G, 128).transpose(0, 1, 3, 2, 4).reshape(R, 3, G, 2048)
    return (gram_matrix, new_basis, offsets)


def solution(mesh):
    split = Mesh(
        mesh.devices.reshape(mesh.shape["grp"], 8, 4, 2), ("grp", "slab_0", "slab_1", "slab_2")
    )
    in_specs = (P(None, None, "grp", SLAB), P(None, None, None, SLAB), P(), P("grp", SLAB))
    out_specs = (P(), P(None, None, None, SLAB), P("grp", SLAB))
    return jax.shard_map(
        per_device, mesh=split, in_specs=in_specs, out_specs=out_specs, check_vma=False
    )
```

```python
import jax
import jax.numpy as jnp
from jax import lax
from jax.experimental import pallas as pl
from jax.experimental.pallas import tpu as pltpu
from jax.sharding import Mesh
from jax.sharding import PartitionSpec as P


PLANE = 512
SLAB = ("slab_0", "slab_1", "slab_2")

R = 64
S = 16
N = R + S
G = 4
COLS = 6144
J = 48
ROWS = 192
VPITCH = J + 8
PITCH = ROWS + 1
WIDE = (R + 1) * PITCH + 7
HIGHEST = lax.Precision.HIGHEST
MIB = 2**20


def vmem(n=1):
    return [pl.BlockSpec(memory_space=pltpu.VMEM) for _ in range(n)]


def smem():
    return pl.BlockSpec(memory_space=pltpu.SMEM)


def hbm(n=1):
    return [pl.BlockSpec(memory_space=pltpu.HBM) for _ in range(n)]


def near(x):
    return pltpu.with_memory_space_constraint(x, pltpu.VMEM)


def far(x):
    return pltpu.with_memory_space_constraint(x, pltpu.HBM)


def live_tile(t, thick, rows):
    return jnp.full((rows, 128), jnp.where(t // 4 < thick, 1, 0), jnp.int32) > 0


def snapshots_body(vel_hbm, snap_ref, vel_ref, sem):
    get = pltpu.make_async_copy(vel_hbm, vel_ref.at[:, 0:J], sem)
    get.start()
    get.wait()
    rows_ref = vel_ref.reshape(S * VPITCH, 128)
    for j in range(J):
        rows = rows_ref[pl.ds(j, S, stride=VPITCH), :]
        snap_ref[:, pl.ds(j * 128, 128)] = rows.astype(jnp.bfloat16)


def snapshots(velocity):
    return pl.pallas_call(
        snapshots_body,
        out_shape=pltpu.VMEM((S, COLS), jnp.bfloat16),
        in_specs=hbm(),
        out_specs=vmem()[0],
        scratch_shapes=[pltpu.VMEM((S, VPITCH, 128), jnp.float32), pltpu.SemaphoreType.DMA(())],
        compiler_params=pltpu.CompilerParams(vmem_limit_bytes=2 * MIB),
        cost_estimate=pl.CostEstimate(flops=2 * 10**9, transcendentals=0, bytes_accessed=10**6),
        name="snapshots",
    )(far(velocity.reshape(S, J, 128)))


def gram_body(thick_ref, basis_ref, snap_ref, wide_ref, part_ref, stack_ref):
    g = lax.axis_index("grp")
    core = lax.axis_index("slab_2")
    place = ((g * 8 + lax.axis_index("slab_0")) * 4 + lax.axis_index("slab_1")) * 2 + core
    thick = thick_ref[0, 0]

    def widen(r, _):
        wide_ref[pl.ds(r * PITCH, ROWS), :] = basis_ref[r].astype(jnp.float32)
        return 0

    lax.fori_loop(0, R, widen, 0, unroll=4)
    for j in range(J):
        rows = wide_ref[pl.ds(j * G + g, R, stride=PITCH), :]
        rows = jnp.where(live_tile(j % 16, thick, R), rows, 0.0)
        stack_ref[0:R, pl.ds(j * 128, 128)] = rows.astype(jnp.bfloat16)
        stack_ref[R:N, pl.ds(j * 128, 128)] = jnp.where(
            live_tile(j % 16, thick, S), snap_ref[:, pl.ds(j * 128, 128)], jnp.zeros((), jnp.bfloat16)
        )
    stack_ref[N:, :] = jnp.zeros((128 - N, COLS), jnp.bfloat16)
    stacked = stack_ref[...]
    gram = lax.dot_general(
        stacked, stacked, (((1,), (1,)), ((), ())), preferred_element_type=jnp.float32
    )
    lane = lax.broadcasted_iota(jnp.int32, (16, 128), 1)
    row = lax.broadcasted_iota(jnp.int32, (16, 128), 0)
    thick_block = jnp.where(row * 16 + lane == place, thick.astype(jnp.float32), 0.0)
    upper = jnp.where(lane < 80, gram[0:16], pltpu.roll(gram[32:48], 48, 1))
    last = jnp.where(lane < 112, pltpu.roll(gram[48:64], 32, 1), pltpu.roll(gram[64:80], 48, 1))
    lower = jnp.where(lane < 16, thick_block, jnp.where(lane < 80, gram[16:32], last))
    part_ref[0, 0:16] = upper
    part_ref[0, 16:32] = lower


def gram_partial(thickness, basis, snap):
    return pl.pallas_call(
        gram_body,
        out_shape=(pltpu.VMEM((WIDE, 128), jnp.float32), pltpu.VMEM((1, 32, 128), jnp.float32)),
        in_specs=[smem()] + vmem(2),
        out_specs=vmem(2),
        scratch_shapes=[pltpu.VMEM((128, COLS), jnp.bfloat16)],
        compiler_params=pltpu.CompilerParams(vmem_limit_bytes=8 * MIB),
        cost_estimate=pl.CostEstimate(flops=10**9, transcendentals=0, bytes_accessed=10**7),
        name="gram",
    )(thickness, near(basis), near(snap))


def tree_sum(pieces):
    while len(pieces) > 1:
        pieces = [sum(pieces[i + 1 : i + 2], pieces[i]) for i in range(0, len(pieces), 2)]
    return pieces[0]


def combine_body(*refs):
    *ins, out_ref = refs
    pieces = [ref[i] for ref in ins for i in range(ref.shape[0])]
    total = tree_sum(pieces)
    for i in range(out_ref.shape[0]):
        out_ref[i] = total


def combine(arrays, copies):
    return pl.pallas_call(
        combine_body,
        out_shape=pltpu.VMEM((copies, 32, 128), jnp.float32),
        in_specs=vmem(len(arrays)),
        out_specs=vmem()[0],
        compiler_params=pltpu.CompilerParams(vmem_limit_bytes=MIB),
        name="combine",
    )(*(near(a) for a in arrays))


def update_body(total_ref, sv_ref, s0, s1, s2, s3, wide_ref, gram_ref, new_ref, off_ref, snap_ref, f_ref, out_ref, sems):
    g = lax.axis_index("grp")
    core = lax.axis_index("slab_2")
    slab = (lax.axis_index("slab_0") * 4 + lax.axis_index("slab_1")) * 2 + core
    place = g * 64 + slab
    for k, ref in enumerate((s0, s1, s2, s3)):
        snap_ref[g ^ k] = ref[...]
    upper, lower = total_ref[0, 0:16], total_ref[0, 16:32]
    lane = lax.broadcasted_iota(jnp.int32, (16, 128), 1)
    row = lax.broadcasted_iota(jnp.int32, (16, 128), 0)
    order = row * 16 + lane
    thick = jnp.where(lane < 16, lower, 0.0)
    before = jnp.sum(jnp.where(order < place, thick, 0.0))
    off_ref[0, 0] = before.astype(jnp.int32)
    live = jnp.sum(thick) * PLANE
    blocks = (
        upper,
        lower,
        pltpu.roll(upper, 128 - 48, 1),
        pltpu.roll(lower, 128 - 32, 1),
        pltpu.roll(lower, 128 - 48, 1),
    )
    diag = [jnp.where((lane >= 16 * i) & (lane < 80), b, 0.0) for i, b in enumerate(blocks)]
    strict = [jnp.where(lane >= 16 * (i + 1), b, 0.0) for i, b in enumerate(diag)]
    pad = [jnp.zeros((48, 128), jnp.float32)]
    raw = jnp.concatenate(diag + pad, 0) + jnp.concatenate(strict + pad, 0).T
    scale_row = jnp.concatenate([sv_ref[...], jnp.ones((1, 128 - R), jnp.float32)], 1)
    scale_cols = jnp.broadcast_to(scale_row, (128, 128))
    scale_rows = scale_cols.T
    full = raw * scale_rows * scale_cols / (3.0 * live)
    gram_ref[...] = full[:N, :N]
    it = full[:R]
    it = it * (0.5 * R**0.5 / jnp.sqrt(jnp.sum(it * it)))
    for _ in range(4):
        prod = lax.dot_general(it, it, (((1,), (1,)), ((), ())), precision=HIGHEST)
        it = 1.5 * it - 0.5 * jnp.dot(prod, it, precision=HIGHEST)
    mix = (it * scale_cols[:R])[:, :N].astype(jnp.bfloat16)
    slab_thick = [
        jnp.sum(jnp.where(order == k * 64 + slab, thick, 0.0)).astype(jnp.int32) for k in range(G)
    ]
    copies = []
    for c in range(3):
        for k in range(G):
            tiles = range(c * 16, c * 16 + 16)
            parts = [wide_ref[pl.ds(j * G + k, R, stride=PITCH), :].astype(jnp.bfloat16) for j in tiles]
            snap = snap_ref[k, :, pl.ds(c * 2048, 2048)]
            stacked = jnp.concatenate([jnp.concatenate(parts, 1), snap], 0)
            res = jnp.dot(mix, stacked, preferred_element_type=jnp.float32)
            for t, j in enumerate(tiles):
                part = jnp.where(live_tile(t, slab_thick[k], R), res[:, t * 128 : (t + 1) * 128], 0.0)
                f_ref[pl.ds(j * G + k, R, stride=PITCH), :] = part

        def narrow(r, _):
            part = f_ref[pl.ds(r * PITCH + c * 64, 64), :]
            out_ref[r, pl.ds(c * 64, 64), :] = part.astype(jnp.bfloat16)
            return 0

        lax.fori_loop(0, R, narrow, 0, unroll=4)
        part = pl.ds(c * 64, 64)
        copy = pltpu.make_async_copy(out_ref.at[:, part], new_ref.at[:, part], sems.at[c])
        copy.start()
        copies.append(copy)
    for copy in copies:
        copy.wait()


def update(total, sv, wide, snaps):
    return pl.pallas_call(
        update_body,
        out_shape=(
            jax.ShapeDtypeStruct((N, N), jnp.float32),
            jax.ShapeDtypeStruct((R, ROWS, 128), jnp.bfloat16),
            jax.ShapeDtypeStruct((1, 1), jnp.int32),
        ),
        in_specs=vmem(7),
        out_specs=(vmem()[0], pl.BlockSpec(memory_space=pl.ANY), smem()),
        scratch_shapes=[
            pltpu.VMEM((G, S, COLS), jnp.bfloat16),
            pltpu.VMEM((WIDE, 128), jnp.float32),
            pltpu.VMEM((R, ROWS, 128), jnp.bfloat16),
            pltpu.SemaphoreType.DMA((3,)),
        ],
        compiler_params=pltpu.CompilerParams(vmem_limit_bytes=20 * MIB),
        name="update",
    )(near(total), near(sv.reshape(1, R)), *(near(s) for s in snaps), near(wide))


def from_region(snap, k):
    return lax.ppermute(snap, "grp", [(i, i ^ k) for i in range(G)])


def per_device(velocity, old_basis, singular_values, thickness):
    basis = old_basis.reshape(R, 3, G, 16, 128).transpose(0, 1, 3, 2, 4).reshape(R, ROWS, 128)
    snap = snapshots(velocity)
    thickness = lax.optimization_barrier((thickness, snap))[0]
    snaps = [snap] + [from_region(snap, k) for k in (1, 2, 3)]
    wide, part = gram_partial(thickness, basis, snap)
    got = lax.ppermute(part, "slab_2", [(0, 1), (1, 0)])
    spread = combine((part, got), 8)
    got = lax.all_to_all(spread, "slab_0", 0, 0, tiled=True)
    got = lax.all_to_all(combine((got,), 16), ("grp", "slab_1"), 0, 0, tiled=True)
    total = combine((got,), 1)
    gram_matrix, new, offsets = update(total, singular_values, wide, snaps)
    new_basis = new.reshape(R, 3, 16, G, 128).transpose(0, 1, 3, 2, 4).reshape(R, 3, G, 2048)
    return (gram_matrix, new_basis, offsets)


def solution(mesh):
    split = Mesh(
        mesh.devices.reshape(mesh.shape["grp"], 8, 4, 2), ("grp", "slab_0", "slab_1", "slab_2")
    )
    in_specs = (P(None, None, "grp", SLAB), P(None, None, None, SLAB), P(), P("grp", SLAB))
    out_specs = (P(), P(None, None, None, SLAB), P("grp", SLAB))
    return jax.shard_map(
        per_device, mesh=split, in_specs=in_specs, out_specs=out_specs, check_vma=False
    )
```

```python
import jax
import jax.numpy as jnp
from jax import lax
from jax.experimental import pallas as pl
from jax.experimental.pallas import tpu as pltpu
from jax.sharding import Mesh
from jax.sharding import PartitionSpec as P


PLANE = 512
SLAB = ("slab_0", "slab_1", "slab_2")

R = 64
S = 16
N = R + S
G = 4
COLS = 6144
J = 48
ROWS = 192
VPITCH = J + 8
PITCH = ROWS + 1
WIDE = (R + 1) * PITCH + 7
HIGHEST = lax.Precision.HIGHEST
MIB = 2**20


def vmem(n=1):
    return [pl.BlockSpec(memory_space=pltpu.VMEM) for _ in range(n)]


def smem():
    return pl.BlockSpec(memory_space=pltpu.SMEM)


def hbm(n=1):
    return [pl.BlockSpec(memory_space=pltpu.HBM) for _ in range(n)]


def near(x):
    return pltpu.with_memory_space_constraint(x, pltpu.VMEM)


def far(x):
    return pltpu.with_memory_space_constraint(x, pltpu.HBM)


def live_tile(t, thick, rows):
    return jnp.full((rows, 128), jnp.where(t // 4 < thick, 1, 0), jnp.int32) > 0


def snapshots_body(vel_hbm, snap_ref, vel_ref, sem):
    get = pltpu.make_async_copy(vel_hbm, vel_ref.at[:, 0:J], sem)
    get.start()
    get.wait()
    rows_ref = vel_ref.reshape(S * VPITCH, 128)
    for j in range(J):
        rows = rows_ref[pl.ds(j, S, stride=VPITCH), :]
        snap_ref[:, pl.ds(j * 128, 128)] = rows.astype(jnp.bfloat16)


def snapshots(velocity):
    return pl.pallas_call(
        snapshots_body,
        out_shape=pltpu.VMEM((S, COLS), jnp.bfloat16),
        in_specs=hbm(),
        out_specs=vmem()[0],
        scratch_shapes=[pltpu.VMEM((S, VPITCH, 128), jnp.float32), pltpu.SemaphoreType.DMA(())],
        compiler_params=pltpu.CompilerParams(vmem_limit_bytes=2 * MIB),
        cost_estimate=pl.CostEstimate(flops=10**9, transcendentals=0, bytes_accessed=10**6),
        name="snapshots",
    )(far(velocity.reshape(S, J, 128)))


def gram_body(thick_ref, basis_ref, snap_ref, part_ref, snap_hbm, wide_ref, stack_ref, sem):
    put = pltpu.make_async_copy(snap_ref, snap_hbm, sem)
    put.start()
    g = lax.axis_index("grp")
    core = lax.axis_index("slab_2")
    place = ((g * 8 + lax.axis_index("slab_0")) * 4 + lax.axis_index("slab_1")) * 2 + core
    thick = thick_ref[0, 0]

    def widen(r, _):
        wide_ref[pl.ds(r * PITCH, ROWS), :] = basis_ref[r].astype(jnp.float32)
        return 0

    lax.fori_loop(0, R, widen, 0, unroll=4)
    for j in range(J):
        rows = wide_ref[pl.ds(j * G + g, R, stride=PITCH), :]
        rows = jnp.where(live_tile(j % 16, thick, R), rows, 0.0)
        stack_ref[0:R, pl.ds(j * 128, 128)] = rows.astype(jnp.bfloat16)
        stack_ref[R:N, pl.ds(j * 128, 128)] = jnp.where(
            live_tile(j % 16, thick, S), snap_ref[:, pl.ds(j * 128, 128)], jnp.zeros((), jnp.bfloat16)
        )
    stack_ref[N:, :] = jnp.zeros((128 - N, COLS), jnp.bfloat16)
    stacked = stack_ref[...]
    gram = lax.dot_general(
        stacked, stacked, (((1,), (1,)), ((), ())), preferred_element_type=jnp.float32
    )
    lane = lax.broadcasted_iota(jnp.int32, (16, 128), 1)
    row = lax.broadcasted_iota(jnp.int32, (16, 128), 0)
    thick_block = jnp.where(row * 16 + lane == place, thick.astype(jnp.float32), 0.0)
    upper = jnp.where(lane < 80, gram[0:16], pltpu.roll(gram[32:48], 48, 1))
    last = jnp.where(lane < 112, pltpu.roll(gram[48:64], 32, 1), pltpu.roll(gram[64:80], 48, 1))
    lower = jnp.where(lane < 16, thick_block, jnp.where(lane < 80, gram[16:32], last))
    part_ref[0, 0:16] = upper
    part_ref[0, 16:32] = lower
    put.wait()


def gram_partial(thickness, basis, snap):
    return pl.pallas_call(
        gram_body,
        out_shape=(pltpu.VMEM((1, 32, 128), jnp.float32), pltpu.HBM((S, COLS), jnp.bfloat16)),
        in_specs=[smem()] + vmem(2),
        out_specs=vmem() + hbm(),
        scratch_shapes=[
            pltpu.VMEM((WIDE, 128), jnp.float32),
            pltpu.VMEM((128, COLS), jnp.bfloat16),
            pltpu.SemaphoreType.DMA(()),
        ],
        compiler_params=pltpu.CompilerParams(vmem_limit_bytes=16 * MIB),
        cost_estimate=pl.CostEstimate(flops=10**9, transcendentals=0, bytes_accessed=10**7),
        name="gram",
    )(thickness, near(basis), near(snap))


def tree_sum(pieces):
    while len(pieces) > 1:
        pieces = [sum(pieces[i + 1 : i + 2], pieces[i]) for i in range(0, len(pieces), 2)]
    return pieces[0]


def combine_body(*refs):
    *ins, out_ref = refs
    pieces = [ref[i] for ref in ins for i in range(ref.shape[0])]
    total = tree_sum(pieces)
    for i in range(out_ref.shape[0]):
        out_ref[i] = total


def combine(arrays, copies):
    return pl.pallas_call(
        combine_body,
        out_shape=pltpu.VMEM((copies, 32, 128), jnp.float32),
        in_specs=vmem(len(arrays)),
        out_specs=vmem()[0],
        compiler_params=pltpu.CompilerParams(vmem_limit_bytes=MIB),
        name="combine",
    )(*(near(a) for a in arrays))


def spread_body(mine_ref, other_ref, out_hbm, total_ref, sems):
    total_ref[...] = mine_ref[0] + other_ref[0]
    puts = [
        pltpu.make_async_copy(total_ref, out_hbm.at[i], sems.at[i]) for i in range(out_hbm.shape[0])
    ]
    for put in puts:
        put.start()
    for put in puts:
        put.wait()


def spread_far(mine, other, copies):
    return pl.pallas_call(
        spread_body,
        out_shape=pltpu.HBM((copies, 32, 128), jnp.float32),
        in_specs=vmem(2),
        out_specs=hbm()[0],
        scratch_shapes=[pltpu.VMEM((32, 128), jnp.float32), pltpu.SemaphoreType.DMA((copies,))],
        compiler_params=pltpu.CompilerParams(vmem_limit_bytes=MIB),
        name="spread",
    )(near(mine), near(other))


def update_body(total_ref, sv_ref, basis_ref, s0, s1, s2, s3, gram_ref, new_ref, off_ref, snap_ref, wide_ref, f_ref, out_ref, sems):
    g = lax.axis_index("grp")
    core = lax.axis_index("slab_2")
    slab = (lax.axis_index("slab_0") * 4 + lax.axis_index("slab_1")) * 2 + core
    place = g * 64 + slab
    gets = [
        pltpu.make_async_copy(ref, snap_ref.at[g ^ k], sems.at[3 + k])
        for k, ref in enumerate((s0, s1, s2, s3))
    ]
    for get in gets:
        get.start()
    upper, lower = total_ref[0, 0:16], total_ref[0, 16:32]
    lane = lax.broadcasted_iota(jnp.int32, (16, 128), 1)
    row = lax.broadcasted_iota(jnp.int32, (16, 128), 0)
    order = row * 16 + lane
    thick = jnp.where(lane < 16, lower, 0.0)
    before = jnp.sum(jnp.where(order < place, thick, 0.0))
    off_ref[0, 0] = before.astype(jnp.int32)
    live = jnp.sum(thick) * PLANE
    blocks = (
        upper,
        lower,
        pltpu.roll(upper, 128 - 48, 1),
        pltpu.roll(lower, 128 - 32, 1),
        pltpu.roll(lower, 128 - 48, 1),
    )
    diag = [jnp.where((lane >= 16 * i) & (lane < 80), b, 0.0) for i, b in enumerate(blocks)]
    strict = [jnp.where(lane >= 16 * (i + 1), b, 0.0) for i, b in enumerate(diag)]
    pad = [jnp.zeros((48, 128), jnp.float32)]
    raw = jnp.concatenate(diag + pad, 0) + jnp.concatenate(strict + pad, 0).T
    scale_row = jnp.concatenate([sv_ref[...], jnp.ones((1, 128 - R), jnp.float32)], 1)
    scale_cols = jnp.broadcast_to(scale_row, (128, 128))
    scale_rows = scale_cols.T
    full = raw * scale_rows * scale_cols / (3.0 * live)
    gram_ref[...] = full[:N, :N]
    it = full[:R]
    it = it * (0.5 * R**0.5 / jnp.sqrt(jnp.sum(it * it)))
    for i in range(4):
        if i == 3:
            for get in gets:
                get.wait()
        for r in range(i * 16, i * 16 + 16):
            wide_ref[pl.ds(r * PITCH, ROWS), :] = basis_ref[r].astype(jnp.float32)
        prod = lax.dot_general(it, it, (((1,), (1,)), ((), ())), precision=HIGHEST)
        it = 1.5 * it - 0.5 * jnp.dot(prod, it, precision=HIGHEST)
    mix = (it * scale_cols[:R])[:, :N].astype(jnp.bfloat16)
    slab_thick = [
        jnp.sum(jnp.where(order == k * 64 + slab, thick, 0.0)).astype(jnp.int32) for k in range(G)
    ]
    copies = []
    for c in range(3):
        for k in range(G):
            tiles = range(c * 16, c * 16 + 16)
            parts = [wide_ref[pl.ds(j * G + k, R, stride=PITCH), :].astype(jnp.bfloat16) for j in tiles]
            snap = snap_ref[k, :, pl.ds(c * 2048, 2048)]
            stacked = jnp.concatenate([jnp.concatenate(parts, 1), snap], 0)
            res = jnp.dot(mix, stacked, preferred_element_type=jnp.float32)
            for t, j in enumerate(tiles):
                part = jnp.where(live_tile(t, slab_thick[k], R), res[:, t * 128 : (t + 1) * 128], 0.0)
                f_ref[pl.ds(j * G + k, R, stride=PITCH), :] = part

        def narrow(r, _):
            part = f_ref[pl.ds(r * PITCH + c * 64, 64), :]
            out_ref[r, pl.ds(c * 64, 64), :] = part.astype(jnp.bfloat16)
            return 0

        lax.fori_loop(0, R, narrow, 0, unroll=4)
        part = pl.ds(c * 64, 64)
        copy = pltpu.make_async_copy(out_ref.at[:, part], new_ref.at[:, part], sems.at[c])
        copy.start()
        copies.append(copy)
    for copy in copies:
        copy.wait()


def update(total, sv, basis, snaps):
    return pl.pallas_call(
        update_body,
        out_shape=(
            jax.ShapeDtypeStruct((N, N), jnp.float32),
            jax.ShapeDtypeStruct((R, ROWS, 128), jnp.bfloat16),
            jax.ShapeDtypeStruct((1, 1), jnp.int32),
        ),
        in_specs=vmem(3) + hbm(4),
        out_specs=(vmem()[0], pl.BlockSpec(memory_space=pl.ANY), smem()),
        scratch_shapes=[
            pltpu.VMEM((G, S, COLS), jnp.bfloat16),
            pltpu.VMEM((WIDE, 128), jnp.float32),
            pltpu.VMEM((WIDE, 128), jnp.float32),
            pltpu.VMEM((R, ROWS, 128), jnp.bfloat16),
            pltpu.SemaphoreType.DMA((7,)),
        ],
        compiler_params=pltpu.CompilerParams(vmem_limit_bytes=28 * MIB),
        name="update",
    )(near(total), near(sv.reshape(1, R)), near(basis), *(far(s) for s in snaps))


def from_region(snap, k):
    return lax.ppermute(snap, "grp", [(i, i ^ k) for i in range(G)])


def per_device(velocity, old_basis, singular_values, thickness):
    basis = old_basis.reshape(R, 3, G, 16, 128).transpose(0, 1, 3, 2, 4).reshape(R, ROWS, 128)
    snap = snapshots(velocity)
    thickness = lax.optimization_barrier((thickness, snap))[0]
    part, snap = gram_partial(thickness, basis, snap)
    snaps = [snap] + [from_region(snap, k) for k in (1, 2, 3)]
    got = lax.ppermute(part, "slab_2", [(0, 1), (1, 0)])
    spread = spread_far(part, got, 16)
    got = lax.all_to_all(spread, ("grp", "slab_1"), 0, 0, tiled=True)
    spread = combine((got,), 8)
    got = lax.all_to_all(spread, "slab_0", 0, 0, tiled=True)
    total = combine((got,), 1)
    gram_matrix, new, offsets = update(total, singular_values, basis, snaps)
    new_basis = new.reshape(R, 3, 16, G, 128).transpose(0, 1, 3, 2, 4).reshape(R, 3, G, 2048)
    return (gram_matrix, new_basis, offsets)


def solution(mesh):
    split = Mesh(
        mesh.devices.reshape(mesh.shape["grp"], 8, 4, 2), ("grp", "slab_0", "slab_1", "slab_2")
    )
    in_specs = (P(None, None, "grp", SLAB), P(None, None, None, SLAB), P(), P("grp", SLAB))
    out_specs = (P(), P(None, None, None, SLAB), P("grp", SLAB))
    return jax.shard_map(
        per_device, mesh=split, in_specs=in_specs, out_specs=out_specs, check_vma=False
    )
```

```python
import jax
import jax.numpy as jnp
from jax import lax
from jax.experimental import pallas as pl
from jax.experimental.pallas import tpu as pltpu
from jax.sharding import Mesh
from jax.sharding import PartitionSpec as P


PLANE = 512
SLAB = ("slab_0", "slab_1", "slab_2")

R = 64
S = 16
N = R + S
G = 4
COLS = 6144
J = 48
ROWS = 192
VPITCH = J + 8
PITCH = ROWS + 1
WIDE = (R + 1) * PITCH + 7
HIGHEST = lax.Precision.HIGHEST
MIB = 2**20


def vmem(n=1):
    return [pl.BlockSpec(memory_space=pltpu.VMEM) for _ in range(n)]


def smem():
    return pl.BlockSpec(memory_space=pltpu.SMEM)


def hbm(n=1):
    return [pl.BlockSpec(memory_space=pltpu.HBM) for _ in range(n)]


def near(x):
    return pltpu.with_memory_space_constraint(x, pltpu.VMEM)


def far(x):
    return pltpu.with_memory_space_constraint(x, pltpu.HBM)


def live_tile(t, thick, rows):
    return jnp.full((rows, 128), jnp.where(t // 4 < thick, 1, 0), jnp.int32) > 0


def snapshots_body(vel_hbm, snap_ref, vel_ref, sem):
    get = pltpu.make_async_copy(vel_hbm, vel_ref.at[:, 0:J], sem)
    get.start()
    get.wait()
    rows_ref = vel_ref.reshape(S * VPITCH, 128)
    for j in range(J):
        rows = rows_ref[pl.ds(j, S, stride=VPITCH), :]
        snap_ref[:, pl.ds(j * 128, 128)] = rows.astype(jnp.bfloat16)


def snapshots(velocity):
    return pl.pallas_call(
        snapshots_body,
        out_shape=pltpu.VMEM((S, COLS), jnp.bfloat16),
        in_specs=hbm(),
        out_specs=vmem()[0],
        scratch_shapes=[pltpu.VMEM((S, VPITCH, 128), jnp.float32), pltpu.SemaphoreType.DMA(())],
        compiler_params=pltpu.CompilerParams(vmem_limit_bytes=2 * MIB),
        cost_estimate=pl.CostEstimate(flops=10**9, transcendentals=0, bytes_accessed=10**6),
        name="snapshots",
    )(far(velocity.reshape(S, J, 128)))


def gram_body(thick_ref, basis_ref, snap_ref, part_ref, wide_ref, stack_ref):
    g = lax.axis_index("grp")
    core = lax.axis_index("slab_2")
    place = ((g * 8 + lax.axis_index("slab_0")) * 4 + lax.axis_index("slab_1")) * 2 + core
    thick = thick_ref[0, 0]

    def widen(r, _):
        wide_ref[pl.ds(r * PITCH, ROWS), :] = basis_ref[r].astype(jnp.float32)
        return 0

    lax.fori_loop(0, R, widen, 0, unroll=4)
    for j in range(J):
        rows = wide_ref[pl.ds(j * G + g, R, stride=PITCH), :]
        rows = jnp.where(live_tile(j % 16, thick, R), rows, 0.0)
        stack_ref[0:R, pl.ds(j * 128, 128)] = rows.astype(jnp.bfloat16)
        stack_ref[R:N, pl.ds(j * 128, 128)] = jnp.where(
            live_tile(j % 16, thick, S), snap_ref[:, pl.ds(j * 128, 128)], jnp.zeros((), jnp.bfloat16)
        )
    stack_ref[N:, :] = jnp.zeros((128 - N, COLS), jnp.bfloat16)
    stacked = stack_ref[...]
    gram = lax.dot_general(
        stacked, stacked, (((1,), (1,)), ((), ())), preferred_element_type=jnp.float32
    )
    lane = lax.broadcasted_iota(jnp.int32, (16, 128), 1)
    row = lax.broadcasted_iota(jnp.int32, (16, 128), 0)
    thick_block = jnp.where(row * 16 + lane == place, thick.astype(jnp.float32), 0.0)
    upper = jnp.where(lane < 80, gram[0:16], pltpu.roll(gram[32:48], 48, 1))
    last = jnp.where(lane < 112, pltpu.roll(gram[48:64], 32, 1), pltpu.roll(gram[64:80], 48, 1))
    lower = jnp.where(lane < 16, thick_block, jnp.where(lane < 80, gram[16:32], last))
    part_ref[0, 0:16] = upper
    part_ref[0, 16:32] = lower


def gram_partial(thickness, basis, snap):
    return pl.pallas_call(
        gram_body,
        out_shape=pltpu.VMEM((1, 32, 128), jnp.float32),
        in_specs=[smem()] + vmem(2),
        out_specs=vmem()[0],
        scratch_shapes=[pltpu.VMEM((WIDE, 128), jnp.float32), pltpu.VMEM((128, COLS), jnp.bfloat16)],
        compiler_params=pltpu.CompilerParams(vmem_limit_bytes=16 * MIB),
        cost_estimate=pl.CostEstimate(flops=10**9, transcendentals=0, bytes_accessed=10**7),
        name="gram",
    )(thickness, near(basis), near(snap))


def tree_sum(pieces):
    while len(pieces) > 1:
        pieces = [sum(pieces[i + 1 : i + 2], pieces[i]) for i in range(0, len(pieces), 2)]
    return pieces[0]


def combine_body(*refs):
    *ins, out_ref = refs
    pieces = [ref[i] for ref in ins for i in range(ref.shape[0])]
    total = tree_sum(pieces)
    for i in range(out_ref.shape[0]):
        out_ref[i] = total


def combine(arrays, copies):
    return pl.pallas_call(
        combine_body,
        out_shape=pltpu.VMEM((copies, 32, 128), jnp.float32),
        in_specs=vmem(len(arrays)),
        out_specs=vmem()[0],
        compiler_params=pltpu.CompilerParams(vmem_limit_bytes=MIB),
        name="combine",
    )(*(near(a) for a in arrays))


def update_body(total_ref, sv_ref, basis_ref, s0, s1, s2, s3, gram_ref, new_ref, off_ref, snap_ref, wide_ref, f_ref, out_ref, sems):
    g = lax.axis_index("grp")
    core = lax.axis_index("slab_2")
    slab = (lax.axis_index("slab_0") * 4 + lax.axis_index("slab_1")) * 2 + core
    place = g * 64 + slab
    gets = [
        pltpu.make_async_copy(ref, snap_ref.at[g ^ k], sems.at[3 + k])
        for k, ref in enumerate((s0, s1, s2, s3))
    ]
    for get in gets:
        get.start()
    upper, lower = total_ref[0, 0:16], total_ref[0, 16:32]
    lane = lax.broadcasted_iota(jnp.int32, (16, 128), 1)
    row = lax.broadcasted_iota(jnp.int32, (16, 128), 0)
    order = row * 16 + lane
    thick = jnp.where(lane < 16, lower, 0.0)
    before = jnp.sum(jnp.where(order < place, thick, 0.0))
    off_ref[0, 0] = before.astype(jnp.int32)
    live = jnp.sum(thick) * PLANE
    blocks = (
        upper,
        lower,
        pltpu.roll(upper, 128 - 48, 1),
        pltpu.roll(lower, 128 - 32, 1),
        pltpu.roll(lower, 128 - 48, 1),
    )
    diag = [jnp.where((lane >= 16 * i) & (lane < 80), b, 0.0) for i, b in enumerate(blocks)]
    strict = [jnp.where(lane >= 16 * (i + 1), b, 0.0) for i, b in enumerate(diag)]
    pad = [jnp.zeros((48, 128), jnp.float32)]
    raw = jnp.concatenate(diag + pad, 0) + jnp.concatenate(strict + pad, 0).T
    scale_row = jnp.concatenate([sv_ref[...], jnp.ones((1, 128 - R), jnp.float32)], 1)
    scale_cols = jnp.broadcast_to(scale_row, (128, 128))
    scale_rows = scale_cols.T
    full = raw * scale_rows * scale_cols / (3.0 * live)
    gram_ref[...] = full[:N, :N]
    it = full[:R]
    it = it * (0.5 * R**0.5 / jnp.sqrt(jnp.sum(it * it)))
    for i in range(4):
        if i == 3:
            for get in gets:
                get.wait()
        for r in range(i * 16, i * 16 + 16):
            wide_ref[pl.ds(r * PITCH, ROWS), :] = basis_ref[r].astype(jnp.float32)
        prod = lax.dot_general(it, it, (((1,), (1,)), ((), ())), precision=HIGHEST)
        it = 1.5 * it - 0.5 * jnp.dot(prod, it, precision=HIGHEST)
    mix = (it * scale_cols[:R])[:, :N].astype(jnp.bfloat16)
    slab_thick = [
        jnp.sum(jnp.where(order == k * 64 + slab, thick, 0.0)).astype(jnp.int32) for k in range(G)
    ]
    copies = []
    for c in range(3):
        for k in range(G):
            tiles = range(c * 16, c * 16 + 16)
            parts = [wide_ref[pl.ds(j * G + k, R, stride=PITCH), :].astype(jnp.bfloat16) for j in tiles]
            snap = snap_ref[k, :, pl.ds(c * 2048, 2048)]
            stacked = jnp.concatenate([jnp.concatenate(parts, 1), snap], 0)
            res = jnp.dot(mix, stacked, preferred_element_type=jnp.float32)
            for t, j in enumerate(tiles):
                part = jnp.where(live_tile(t, slab_thick[k], R), res[:, t * 128 : (t + 1) * 128], 0.0)
                f_ref[pl.ds(j * G + k, R, stride=PITCH), :] = part

        def narrow(r, _):
            part = f_ref[pl.ds(r * PITCH + c * 64, 64), :]
            out_ref[r, pl.ds(c * 64, 64), :] = part.astype(jnp.bfloat16)
            return 0

        lax.fori_loop(0, R, narrow, 0, unroll=4)
        part = pl.ds(c * 64, 64)
        copy = pltpu.make_async_copy(out_ref.at[:, part], new_ref.at[:, part], sems.at[c])
        copy.start()
        copies.append(copy)
    for copy in copies:
        copy.wait()


def update(total, sv, basis, snaps):
    return pl.pallas_call(
        update_body,
        out_shape=(
            jax.ShapeDtypeStruct((N, N), jnp.float32),
            jax.ShapeDtypeStruct((R, ROWS, 128), jnp.bfloat16),
            jax.ShapeDtypeStruct((1, 1), jnp.int32),
        ),
        in_specs=vmem(3) + hbm(4),
        out_specs=(vmem()[0], pl.BlockSpec(memory_space=pl.ANY), smem()),
        scratch_shapes=[
            pltpu.VMEM((G, S, COLS), jnp.bfloat16),
            pltpu.VMEM((WIDE, 128), jnp.float32),
            pltpu.VMEM((WIDE, 128), jnp.float32),
            pltpu.VMEM((R, ROWS, 128), jnp.bfloat16),
            pltpu.SemaphoreType.DMA((7,)),
        ],
        compiler_params=pltpu.CompilerParams(vmem_limit_bytes=28 * MIB),
        name="update",
    )(near(total), near(sv.reshape(1, R)), near(basis), *(far(s) for s in snaps))


def from_region(snap, k):
    return lax.ppermute(snap, "grp", [(i, i ^ k) for i in range(G)])


def per_device(velocity, old_basis, singular_values, thickness):
    basis = old_basis.reshape(R, 3, G, 16, 128).transpose(0, 1, 3, 2, 4).reshape(R, ROWS, 128)
    snap = snapshots(velocity)
    thickness = lax.optimization_barrier((thickness, snap))[0]
    snaps = [snap] + [from_region(snap, k) for k in (1, 2, 3)]
    part = gram_partial(thickness, basis, snap)
    got = lax.ppermute(part, "slab_2", [(0, 1), (1, 0)])
    spread = combine((part, got), 8)
    got = lax.all_to_all(spread, "slab_0", 0, 0, tiled=True)
    spread = combine((got,), 16)
    got = lax.all_to_all(spread, ("grp", "slab_1"), 0, 0, tiled=True)
    total = combine((got,), 1)
    gram_matrix, new, offsets = update(total, singular_values, basis, snaps)
    new_basis = new.reshape(R, 3, 16, G, 128).transpose(0, 1, 3, 2, 4).reshape(R, 3, G, 2048)
    return (gram_matrix, new_basis, offsets)


def solution(mesh):
    split = Mesh(
        mesh.devices.reshape(mesh.shape["grp"], 8, 4, 2), ("grp", "slab_0", "slab_1", "slab_2")
    )
    in_specs = (P(None, None, "grp", SLAB), P(None, None, None, SLAB), P(), P("grp", SLAB))
    out_specs = (P(), P(None, None, None, SLAB), P("grp", SLAB))
    return jax.shard_map(
        per_device, mesh=split, in_specs=in_specs, out_specs=out_specs, check_vma=False
    )
```

```python
import jax
import jax.numpy as jnp
from jax import lax
from jax.experimental import pallas as pl
from jax.experimental.pallas import tpu as pltpu
from jax.sharding import Mesh
from jax.sharding import PartitionSpec as P


PLANE = 512
SLAB = ("slab_0", "slab_1", "slab_2")

R = 64
S = 16
N = R + S
G = 4
COLS = 6144
J = 48
ROWS = 192
VPITCH = J + 8
PITCH = ROWS + 1
WIDE = (R + 1) * PITCH + 7
HIGHEST = lax.Precision.HIGHEST
MIB = 2**20


def vmem(n=1):
    return [pl.BlockSpec(memory_space=pltpu.VMEM) for _ in range(n)]


def smem():
    return pl.BlockSpec(memory_space=pltpu.SMEM)


def hbm(n=1):
    return [pl.BlockSpec(memory_space=pltpu.HBM) for _ in range(n)]


def near(x):
    return pltpu.with_memory_space_constraint(x, pltpu.VMEM)


def far(x):
    return pltpu.with_memory_space_constraint(x, pltpu.HBM)


def live_tile(t, thick, rows):
    return jnp.full((rows, 128), jnp.where(t // 4 < thick, 1, 0), jnp.int32) > 0


def snapshots_body(vel_hbm, snap_ref, vel_ref, sem):
    get = pltpu.make_async_copy(vel_hbm, vel_ref.at[:, 0:J], sem)
    get.start()
    get.wait()
    rows_ref = vel_ref.reshape(S * VPITCH, 128)
    for j in range(J):
        rows = rows_ref[pl.ds(j, S, stride=VPITCH), :]
        snap_ref[:, pl.ds(j * 128, 128)] = rows.astype(jnp.bfloat16)


def snapshots(velocity):
    return pl.pallas_call(
        snapshots_body,
        out_shape=pltpu.VMEM((S, COLS), jnp.bfloat16),
        in_specs=hbm(),
        out_specs=vmem()[0],
        scratch_shapes=[pltpu.VMEM((S, VPITCH, 128), jnp.float32), pltpu.SemaphoreType.DMA(())],
        compiler_params=pltpu.CompilerParams(vmem_limit_bytes=2 * MIB),
        cost_estimate=pl.CostEstimate(flops=10**9, transcendentals=0, bytes_accessed=10**6),
        name="snapshots",
    )(far(velocity.reshape(S, J, 128)))


def gram_body(thick_ref, basis_ref, snap_ref, part_ref, wide_ref, stack_ref):
    g = lax.axis_index("grp")
    core = lax.axis_index("slab_2")
    place = ((g * 8 + lax.axis_index("slab_0")) * 4 + lax.axis_index("slab_1")) * 2 + core
    thick = thick_ref[0, 0]

    def widen(r, _):
        wide_ref[pl.ds(r * PITCH, ROWS), :] = basis_ref[r].astype(jnp.float32)
        return 0

    lax.fori_loop(0, R, widen, 0, unroll=4)
    for j in range(J):
        rows = wide_ref[pl.ds(j * G + g, R, stride=PITCH), :]
        rows = jnp.where(live_tile(j % 16, thick, R), rows, 0.0)
        stack_ref[0:R, pl.ds(j * 128, 128)] = rows.astype(jnp.bfloat16)
        stack_ref[R:N, pl.ds(j * 128, 128)] = jnp.where(
            live_tile(j % 16, thick, S), snap_ref[:, pl.ds(j * 128, 128)], jnp.zeros((), jnp.bfloat16)
        )
    stack_ref[N:, :] = jnp.zeros((128 - N, COLS), jnp.bfloat16)
    stacked = stack_ref[...]
    gram = lax.dot_general(
        stacked, stacked, (((1,), (1,)), ((), ())), preferred_element_type=jnp.float32
    )
    lane = lax.broadcasted_iota(jnp.int32, (16, 128), 1)
    row = lax.broadcasted_iota(jnp.int32, (16, 128), 0)
    thick_block = jnp.where(row * 16 + lane == place, thick.astype(jnp.float32), 0.0)
    upper = jnp.where(lane < 80, gram[0:16], pltpu.roll(gram[32:48], 48, 1))
    last = jnp.where(lane < 112, pltpu.roll(gram[48:64], 32, 1), pltpu.roll(gram[64:80], 48, 1))
    lower = jnp.where(lane < 16, thick_block, jnp.where(lane < 80, gram[16:32], last))
    part_ref[0, 0:16] = upper
    part_ref[0, 16:32] = lower


def gram_partial(thickness, basis, snap):
    return pl.pallas_call(
        gram_body,
        out_shape=pltpu.VMEM((1, 32, 128), jnp.float32),
        in_specs=[smem()] + vmem(2),
        out_specs=vmem()[0],
        scratch_shapes=[pltpu.VMEM((WIDE, 128), jnp.float32), pltpu.VMEM((128, COLS), jnp.bfloat16)],
        compiler_params=pltpu.CompilerParams(vmem_limit_bytes=16 * MIB),
        cost_estimate=pl.CostEstimate(flops=10**9, transcendentals=0, bytes_accessed=10**7),
        name="gram",
    )(thickness, near(basis), near(snap))


def tree_sum(pieces):
    while len(pieces) > 1:
        pieces = [sum(pieces[i + 1 : i + 2], pieces[i]) for i in range(0, len(pieces), 2)]
    return pieces[0]


def combine_body(*refs):
    *ins, out_ref = refs
    pieces = [ref[i] for ref in ins for i in range(ref.shape[0])]
    total = tree_sum(pieces)
    for i in range(out_ref.shape[0]):
        out_ref[i] = total


def combine(arrays, copies):
    return pl.pallas_call(
        combine_body,
        out_shape=pltpu.VMEM((copies, 32, 128), jnp.float32),
        in_specs=vmem(len(arrays)),
        out_specs=vmem()[0],
        compiler_params=pltpu.CompilerParams(vmem_limit_bytes=MIB),
        name="combine",
    )(*(near(a) for a in arrays))


def update_body(total_ref, sv_ref, basis_ref, s0, s1, s2, s3, gram_ref, new_ref, off_ref, snap_ref, wide_ref, f_ref, out_ref, sems):
    g = lax.axis_index("grp")
    core = lax.axis_index("slab_2")
    slab = (lax.axis_index("slab_0") * 4 + lax.axis_index("slab_1")) * 2 + core
    place = g * 64 + slab
    gets = [
        pltpu.make_async_copy(ref, snap_ref.at[g ^ k], sems.at[12 + k])
        for k, ref in enumerate((s0, s1, s2, s3))
    ]
    for get in gets:
        get.start()
    upper, lower = total_ref[0, 0:16], total_ref[0, 16:32]
    lane = lax.broadcasted_iota(jnp.int32, (16, 128), 1)
    row = lax.broadcasted_iota(jnp.int32, (16, 128), 0)
    order = row * 16 + lane
    thick = jnp.where(lane < 16, lower, 0.0)
    before = jnp.sum(jnp.where(order < place, thick, 0.0))
    off_ref[0, 0] = before.astype(jnp.int32)
    live = jnp.sum(thick) * PLANE
    blocks = (
        upper,
        lower,
        pltpu.roll(upper, 128 - 48, 1),
        pltpu.roll(lower, 128 - 32, 1),
        pltpu.roll(lower, 128 - 48, 1),
    )
    diag = [jnp.where((lane >= 16 * i) & (lane < 80), b, 0.0) for i, b in enumerate(blocks)]
    strict = [jnp.where(lane >= 16 * (i + 1), b, 0.0) for i, b in enumerate(diag)]
    pad = [jnp.zeros((48, 128), jnp.float32)]
    raw = jnp.concatenate(diag + pad, 0) + jnp.concatenate(strict + pad, 0).T
    scale_row = jnp.concatenate([sv_ref[...], jnp.ones((1, 128 - R), jnp.float32)], 1)
    scale_cols = jnp.broadcast_to(scale_row, (128, 128))
    scale_rows = scale_cols.T
    full = raw * scale_rows * scale_cols / (3.0 * live)
    gram_ref[...] = full[:N, :N]
    it = full[:R]
    it = it * (0.5 * R**0.5 / jnp.sqrt(jnp.sum(it * it)))
    for i in range(4):
        if i == 3:
            for get in gets:
                get.wait()
        for r in range(i * 16, i * 16 + 16):
            wide_ref[pl.ds(r * PITCH, ROWS), :] = basis_ref[r].astype(jnp.float32)
        prod = lax.dot_general(it, it, (((1,), (1,)), ((), ())), precision=HIGHEST)
        it = 1.5 * it - 0.5 * jnp.dot(prod, it, precision=HIGHEST)
    mix = (it * scale_cols[:R])[:, :N].astype(jnp.bfloat16)
    slab_thick = [
        jnp.sum(jnp.where(order == k * 64 + slab, thick, 0.0)).astype(jnp.int32) for k in range(G)
    ]
    copies = []

    def compute(lo, hi):
        tiles = range(lo, hi)
        for k in range(G):
            parts = [wide_ref[pl.ds(j * G + k, R, stride=PITCH), :].astype(jnp.bfloat16) for j in tiles]
            snap = snap_ref[k, :, pl.ds(lo * 128, (hi - lo) * 128)]
            stacked = jnp.concatenate([jnp.concatenate(parts, 1), snap], 0)
            res = jnp.dot(mix, stacked, preferred_element_type=jnp.float32)
            for t, j in enumerate(tiles):
                part = jnp.where(live_tile(j % 16, slab_thick[k], R), res[:, t * 128 : (t + 1) * 128], 0.0)
                f_ref[pl.ds(j * G + k, R, stride=PITCH), :] = part

    def emit(lo, hi):
        at, rows = lo * G, (hi - lo) * G
        for r in range(R):
            out_ref[r, pl.ds(at, rows), :] = f_ref[pl.ds(r * PITCH + at, rows), :].astype(jnp.bfloat16)
        part = pl.ds(at, rows)
        copy = pltpu.make_async_copy(out_ref.at[:, part], new_ref.at[:, part], sems.at[len(copies)])
        copy.start()
        copies.append(copy)

    compute(0, 8)
    compute(8, 16)
    emit(0, 8)
    compute(16, 24)
    emit(8, 16)
    compute(24, 32)
    emit(16, 24)
    compute(32, 40)
    emit(24, 32)
    compute(40, 48)
    emit(32, 40)
    emit(40, 48)
    for copy in copies:
        copy.wait()


def update(total, sv, basis, snaps):
    return pl.pallas_call(
        update_body,
        out_shape=(
            jax.ShapeDtypeStruct((N, N), jnp.float32),
            jax.ShapeDtypeStruct((R, ROWS, 128), jnp.bfloat16),
            jax.ShapeDtypeStruct((1, 1), jnp.int32),
        ),
        in_specs=vmem(3) + hbm(4),
        out_specs=(vmem()[0], pl.BlockSpec(memory_space=pl.ANY), smem()),
        scratch_shapes=[
            pltpu.VMEM((G, S, COLS), jnp.bfloat16),
            pltpu.VMEM((WIDE, 128), jnp.float32),
            pltpu.VMEM((WIDE, 128), jnp.float32),
            pltpu.VMEM((R, ROWS, 128), jnp.bfloat16),
            pltpu.SemaphoreType.DMA((16,)),
        ],
        compiler_params=pltpu.CompilerParams(vmem_limit_bytes=28 * MIB),
        name="update",
    )(near(total), near(sv.reshape(1, R)), near(basis), *(far(s) for s in snaps))


def from_region(snap, k):
    return lax.ppermute(snap, "grp", [(i, i ^ k) for i in range(G)])


def per_device(velocity, old_basis, singular_values, thickness):
    basis = old_basis.reshape(R, 3, G, 16, 128).transpose(0, 1, 3, 2, 4).reshape(R, ROWS, 128)
    snap = snapshots(velocity)
    thickness = lax.optimization_barrier((thickness, snap))[0]
    snaps = [snap] + [from_region(snap, k) for k in (1, 2, 3)]
    part = gram_partial(thickness, basis, snap)
    got = lax.ppermute(part, "slab_2", [(0, 1), (1, 0)])
    spread = combine((part, got), 8)
    got = lax.all_to_all(spread, "slab_0", 0, 0, tiled=True)
    spread = combine((got,), 16)
    got = lax.all_to_all(spread, ("grp", "slab_1"), 0, 0, tiled=True)
    total = combine((got,), 1)
    gram_matrix, new, offsets = update(total, singular_values, basis, snaps)
    new_basis = new.reshape(R, 3, 16, G, 128).transpose(0, 1, 3, 2, 4).reshape(R, 3, G, 2048)
    return (gram_matrix, new_basis, offsets)


def solution(mesh):
    split = Mesh(
        mesh.devices.reshape(mesh.shape["grp"], 8, 4, 2), ("grp", "slab_0", "slab_1", "slab_2")
    )
    in_specs = (P(None, None, "grp", SLAB), P(None, None, None, SLAB), P(), P("grp", SLAB))
    out_specs = (P(), P(None, None, None, SLAB), P("grp", SLAB))
    return jax.shard_map(
        per_device, mesh=split, in_specs=in_specs, out_specs=out_specs, check_vma=False
    )
```

```python
import jax
import jax.numpy as jnp
from jax import lax
from jax.experimental import pallas as pl
from jax.experimental.pallas import tpu as pltpu
from jax.sharding import Mesh
from jax.sharding import PartitionSpec as P


PLANE = 512
SLAB = ("slab_0", "slab_1", "slab_2")

R = 64
S = 16
N = R + S
G = 4
COLS = 6144
J = 48
ROWS = 192
VPITCH = J + 8
PITCH = ROWS + 1
WIDE = (R + 1) * PITCH + 7
HIGHEST = lax.Precision.HIGHEST
MIB = 2**20


def vmem(n=1):
    return [pl.BlockSpec(memory_space=pltpu.VMEM) for _ in range(n)]


def smem():
    return pl.BlockSpec(memory_space=pltpu.SMEM)


def hbm(n=1):
    return [pl.BlockSpec(memory_space=pltpu.HBM) for _ in range(n)]


def near(x):
    return pltpu.with_memory_space_constraint(x, pltpu.VMEM)


def far(x):
    return pltpu.with_memory_space_constraint(x, pltpu.HBM)


def live_tile(t, thick, rows):
    return jnp.full((rows, 128), jnp.where(t // 4 < thick, 1, 0), jnp.int32) > 0


def snapshots_body(vel_hbm, snap_ref, vel_ref, sem):
    get = pltpu.make_async_copy(vel_hbm, vel_ref.at[:, 0:J], sem)
    get.start()
    get.wait()
    rows_ref = vel_ref.reshape(S * VPITCH, 128)
    for j in range(J):
        rows = rows_ref[pl.ds(j, S, stride=VPITCH), :]
        snap_ref[:, pl.ds(j * 128, 128)] = rows.astype(jnp.bfloat16)


def snapshots(velocity):
    return pl.pallas_call(
        snapshots_body,
        out_shape=pltpu.VMEM((S, COLS), jnp.bfloat16),
        in_specs=hbm(),
        out_specs=vmem()[0],
        scratch_shapes=[pltpu.VMEM((S, VPITCH, 128), jnp.float32), pltpu.SemaphoreType.DMA(())],
        compiler_params=pltpu.CompilerParams(vmem_limit_bytes=2 * MIB),
        cost_estimate=pl.CostEstimate(flops=10**9, transcendentals=0, bytes_accessed=10**6),
        name="snapshots",
    )(far(velocity.reshape(S, J, 128)))


def gram_body(thick_ref, basis_ref, snap_ref, part_hbm, wide_ref, part_ref, sems):
    g = lax.axis_index("grp")
    core = lax.axis_index("slab_2")
    place = ((g * 8 + lax.axis_index("slab_0")) * 4 + lax.axis_index("slab_1")) * 2 + core
    thick = thick_ref[0, 0]

    def widen(r, _):
        wide_ref[pl.ds(r * PITCH, ROWS), :] = basis_ref[r].astype(jnp.float32)
        return 0

    lax.fori_loop(0, R, widen, 0, unroll=4)
    gram = jnp.zeros((N, N), jnp.float32)
    for lo in range(0, J, 48):
        parts = []
        for j in range(lo, lo + 48):
            rows = wide_ref[pl.ds(j * G + g, R, stride=PITCH), :].astype(jnp.bfloat16)
            both = jnp.concatenate([rows, snap_ref[:, pl.ds(j * 128, 128)]], 0)
            parts.append(jnp.where(live_tile(j % 16, thick, N), both, jnp.zeros((), jnp.bfloat16)))
        stacked = jnp.concatenate(parts, 1)
        gram += lax.dot_general(
            stacked, stacked, (((1,), (1,)), ((), ())), preferred_element_type=jnp.float32
        )
    gram = jnp.concatenate([gram, jnp.zeros((N, 128 - N), jnp.float32)], 1)
    lane = lax.broadcasted_iota(jnp.int32, (16, 128), 1)
    row = lax.broadcasted_iota(jnp.int32, (16, 128), 0)
    thick_block = jnp.where(row * 16 + lane == place, thick.astype(jnp.float32), 0.0)
    upper = jnp.where(lane < 80, gram[0:16], pltpu.roll(gram[32:48], 48, 1))
    last = jnp.where(lane < 112, pltpu.roll(gram[48:64], 32, 1), pltpu.roll(gram[64:80], 48, 1))
    lower = jnp.where(lane < 16, thick_block, jnp.where(lane < 80, gram[16:32], last))
    part_ref[0:16] = upper
    part_ref[16:32] = lower
    puts = [pltpu.make_async_copy(part_ref, part_hbm.at[i], sems.at[i]) for i in range(8)]
    for put in puts:
        put.start()
    for put in puts:
        put.wait()


def gram_partial(thickness, basis, snap):
    return pl.pallas_call(
        gram_body,
        out_shape=pltpu.HBM((8, 32, 128), jnp.float32),
        in_specs=[smem()] + vmem(2),
        out_specs=hbm()[0],
        scratch_shapes=[
            pltpu.VMEM((WIDE, 128), jnp.float32),
            pltpu.VMEM((32, 128), jnp.float32),
            pltpu.SemaphoreType.DMA((8,)),
        ],
        compiler_params=pltpu.CompilerParams(vmem_limit_bytes=16 * MIB),
        cost_estimate=pl.CostEstimate(flops=10**9, transcendentals=0, bytes_accessed=10**7),
        name="gram",
    )(thickness, near(basis), near(snap))


def tree_sum(pieces):
    while len(pieces) > 1:
        pieces = [sum(pieces[i + 1 : i + 2], pieces[i]) for i in range(0, len(pieces), 2)]
    return pieces[0]


def combine_body(*refs):
    *ins, out_ref = refs
    pieces = [ref[i] for ref in ins for i in range(ref.shape[0])]
    total = tree_sum(pieces)
    for i in range(out_ref.shape[0]):
        out_ref[i] = total


def combine(arrays, copies):
    return pl.pallas_call(
        combine_body,
        out_shape=pltpu.VMEM((copies, 32, 128), jnp.float32),
        in_specs=vmem(len(arrays)),
        out_specs=vmem()[0],
        compiler_params=pltpu.CompilerParams(vmem_limit_bytes=MIB),
        name="combine",
    )(*(near(a) for a in arrays))


def whole_sum(x):
    return jnp.sum(x, keepdims=True)


def update_body(total_ref, sv_ref, basis_ref, s0, s1, s2, s3, gram_hbm, new_ref, off_hbm, snap_ref, wide_ref, f_ref, out_ref, gram_ref, off_ref, sems):
    g = lax.axis_index("grp")
    core = lax.axis_index("slab_2")
    slab = (lax.axis_index("slab_0") * 4 + lax.axis_index("slab_1")) * 2 + core
    place = g * 64 + slab
    gets = [
        pltpu.make_async_copy(ref, snap_ref.at[g ^ k], sems.at[12 + k])
        for k, ref in enumerate((s0, s1, s2, s3))
    ]
    for get in gets:
        get.start()
    upper, lower = total_ref[0, 0:16], total_ref[0, 16:32]
    lane = lax.broadcasted_iota(jnp.int32, (16, 128), 1)
    row = lax.broadcasted_iota(jnp.int32, (16, 128), 0)
    order = row * 16 + lane
    thick = jnp.where(lane < 16, lower, 0.0)
    off_ref[...] = whole_sum(jnp.where(order < place, thick, 0.0)).astype(jnp.int32)
    put_off = pltpu.make_async_copy(off_ref, off_hbm, sems.at[17])
    put_off.start()
    live = whole_sum(thick) * PLANE
    blocks = (
        upper,
        lower,
        pltpu.roll(upper, 128 - 48, 1),
        pltpu.roll(lower, 128 - 32, 1),
        pltpu.roll(lower, 128 - 48, 1),
    )
    diag = [jnp.where((lane >= 16 * i) & (lane < 80), b, 0.0) for i, b in enumerate(blocks)]
    strict = [jnp.where(lane >= 16 * (i + 1), b, 0.0) for i, b in enumerate(diag)]
    pad = [jnp.zeros((48, 128), jnp.float32)]
    raw = jnp.concatenate(diag + pad, 0) + jnp.concatenate(strict + pad, 0).T
    scale_row = jnp.concatenate([sv_ref[...], jnp.ones((1, 128 - R), jnp.float32)], 1)
    scale_cols = jnp.broadcast_to(scale_row, (128, 128))
    scale_rows = scale_cols.T
    full = raw * scale_rows * scale_cols / (3.0 * live)
    gram_ref[...] = full[:N, :N]
    put_gram = pltpu.make_async_copy(gram_ref, gram_hbm, sems.at[16])
    put_gram.start()
    it = full[:R]
    it = it * (0.5 * R**0.5 / jnp.sqrt(whole_sum(it * it)))
    for i in range(4):
        if i == 3:
            for get in gets:
                get.wait()
        for r in range(i * 16, i * 16 + 16):
            wide_ref[pl.ds(r * PITCH, ROWS), :] = basis_ref[r].astype(jnp.float32)
        prod = lax.dot_general(it, it, (((1,), (1,)), ((), ())), precision=HIGHEST)
        it = 1.5 * it - 0.5 * jnp.dot(prod, it, precision=HIGHEST)
    mix = (it * scale_cols[:R])[:, :N].astype(jnp.bfloat16)
    slab_thick = [
        whole_sum(jnp.where(order == k * 64 + slab, thick, 0.0)) for k in range(G)
    ]
    slab_live = [[jnp.broadcast_to(n, (R, 128)) > p for p in range(4)] for n in slab_thick]
    copies = []

    def compute(lo, hi):
        tiles = range(lo, hi)
        for k in range(G):
            parts = [wide_ref[pl.ds(j * G + k, R, stride=PITCH), :].astype(jnp.bfloat16) for j in tiles]
            snap = snap_ref[k, :, pl.ds(lo * 128, (hi - lo) * 128)]
            stacked = jnp.concatenate([jnp.concatenate(parts, 1), snap], 0)
            res = jnp.dot(mix, stacked, preferred_element_type=jnp.float32)
            for t, j in enumerate(tiles):
                part = jnp.where(slab_live[k][j % 16 // 4], res[:, t * 128 : (t + 1) * 128], 0.0)
                f_ref[pl.ds(j * G + k, R, stride=PITCH), :] = part

    def emit(lo, hi):
        at, rows = lo * G, (hi - lo) * G
        for r in range(R):
            out_ref[r, pl.ds(at, rows), :] = f_ref[pl.ds(r * PITCH + at, rows), :].astype(jnp.bfloat16)
        part = pl.ds(at, rows)
        copy = pltpu.make_async_copy(out_ref.at[:, part], new_ref.at[:, part], sems.at[len(copies)])
        copy.start()
        copies.append(copy)

    compute(0, 4)
    compute(4, 8)
    emit(0, 4)
    compute(8, 12)
    emit(4, 8)
    compute(12, 16)
    emit(8, 12)
    compute(16, 20)
    emit(12, 16)
    compute(20, 24)
    emit(16, 20)
    compute(24, 28)
    emit(20, 24)
    compute(28, 32)
    emit(24, 28)
    compute(32, 36)
    emit(28, 32)
    compute(36, 40)
    emit(32, 36)
    compute(40, 44)
    emit(36, 40)
    compute(44, 48)
    emit(40, 44)
    emit(44, 48)
    for copy in copies + [put_gram, put_off]:
        copy.wait()


def update(total, sv, basis, snaps):
    return pl.pallas_call(
        update_body,
        out_shape=(
            jax.ShapeDtypeStruct((N, N), jnp.float32),
            jax.ShapeDtypeStruct((R, ROWS, 128), jnp.bfloat16),
            jax.ShapeDtypeStruct((1, 1), jnp.int32),
        ),
        in_specs=vmem(3) + hbm(4),
        out_specs=[pl.BlockSpec(memory_space=pl.ANY) for _ in range(3)],
        scratch_shapes=[
            pltpu.VMEM((G, S, COLS), jnp.bfloat16),
            pltpu.VMEM((WIDE, 128), jnp.float32),
            pltpu.VMEM((WIDE, 128), jnp.float32),
            pltpu.VMEM((R, ROWS, 128), jnp.bfloat16),
            pltpu.VMEM((N, N), jnp.float32),
            pltpu.VMEM((1, 1), jnp.int32),
            pltpu.SemaphoreType.DMA((18,)),
        ],
        compiler_params=pltpu.CompilerParams(vmem_limit_bytes=28 * MIB),
        name="update",
    )(near(total), near(sv.reshape(1, R)), near(basis), *(far(s) for s in snaps))


def from_region(snap, k):
    return lax.ppermute(snap, "grp", [(i, i ^ k) for i in range(G)])


def per_device(velocity, old_basis, singular_values, thickness):
    basis = old_basis.reshape(R, 3, G, 16, 128).transpose(0, 1, 3, 2, 4).reshape(R, ROWS, 128)
    snap = snapshots(velocity)
    thickness = lax.optimization_barrier((thickness, snap))[0]
    snaps = [snap] + [from_region(snap, k) for k in (1, 2, 3)]
    part = gram_partial(thickness, basis, snap)
    got = lax.all_to_all(part, "slab_0", 0, 0, tiled=True)
    mine = combine((got,), 1)
    other = lax.ppermute(mine, "slab_2", [(0, 1), (1, 0)])
    spread = combine((mine, other), 16)
    got = lax.all_to_all(spread, ("grp", "slab_1"), 0, 0, tiled=True)
    total = combine((got,), 1)
    gram_matrix, new, offsets = update(total, singular_values, basis, snaps)
    new_basis = new.reshape(R, 3, 16, G, 128).transpose(0, 1, 3, 2, 4).reshape(R, 3, G, 2048)
    return (gram_matrix, new_basis, offsets)


def solution(mesh):
    split = Mesh(
        mesh.devices.reshape(mesh.shape["grp"], 8, 4, 2), ("grp", "slab_0", "slab_1", "slab_2")
    )
    in_specs = (P(None, None, "grp", SLAB), P(None, None, None, SLAB), P(), P("grp", SLAB))
    out_specs = (P(), P(None, None, None, SLAB), P("grp", SLAB))
    return jax.shard_map(
        per_device, mesh=split, in_specs=in_specs, out_specs=out_specs, check_vma=False
    )
```

```python
import jax
import jax.numpy as jnp
from jax import lax
from jax.experimental import pallas as pl
from jax.experimental.pallas import tpu as pltpu
from jax.sharding import Mesh
from jax.sharding import PartitionSpec as P


PLANE = 512
SLAB = ("slab_0", "slab_1", "slab_2")

R = 64
S = 16
N = R + S
G = 4
COLS = 6144
J = 48
ROWS = 192
VPITCH = J + 8
PITCH = ROWS + 1
WIDE = (R + 1) * PITCH + 7
HIGHEST = lax.Precision.HIGHEST
MIB = 2**20


def vmem(n=1):
    return [pl.BlockSpec(memory_space=pltpu.VMEM) for _ in range(n)]


def smem():
    return pl.BlockSpec(memory_space=pltpu.SMEM)


def hbm(n=1):
    return [pl.BlockSpec(memory_space=pltpu.HBM) for _ in range(n)]


def near(x):
    return pltpu.with_memory_space_constraint(x, pltpu.VMEM)


def far(x):
    return pltpu.with_memory_space_constraint(x, pltpu.HBM)


def live_tile(t, thick, rows):
    return jnp.full((rows, 128), jnp.where(t // 4 < thick, 1, 0), jnp.int32) > 0


def snapshots_body(vel_hbm, snap_ref, vel_ref, sem):
    get = pltpu.make_async_copy(vel_hbm, vel_ref.at[:, 0:J], sem)
    get.start()
    get.wait()
    rows_ref = vel_ref.reshape(S * VPITCH, 128)
    for j in range(J):
        rows = rows_ref[pl.ds(j, S, stride=VPITCH), :]
        snap_ref[:, pl.ds(j * 128, 128)] = rows.astype(jnp.bfloat16)


def snapshots(velocity):
    return pl.pallas_call(
        snapshots_body,
        out_shape=pltpu.VMEM((S, COLS), jnp.bfloat16),
        in_specs=hbm(),
        out_specs=vmem()[0],
        scratch_shapes=[pltpu.VMEM((S, VPITCH, 128), jnp.float32), pltpu.SemaphoreType.DMA(())],
        compiler_params=pltpu.CompilerParams(vmem_limit_bytes=2 * MIB),
        cost_estimate=pl.CostEstimate(flops=10**9, transcendentals=0, bytes_accessed=10**6),
        name="snapshots",
    )(far(velocity.reshape(S, J, 128)))


def gram_body(thick_ref, basis_ref, snap_ref, part_ref, wide_ref, stack_ref):
    g = lax.axis_index("grp")
    core = lax.axis_index("slab_2")
    place = ((g * 8 + lax.axis_index("slab_0")) * 4 + lax.axis_index("slab_1")) * 2 + core
    thick = thick_ref[0, 0]

    def widen(r, _):
        wide_ref[pl.ds(r * PITCH, ROWS), :] = basis_ref[r].astype(jnp.float32)
        return 0

    lax.fori_loop(0, R, widen, 0, unroll=16)
    gram = jnp.zeros((N, N), jnp.float32)
    for lo in range(0, J, 48):
        parts = []
        for j in range(lo, lo + 48):
            rows = wide_ref[pl.ds(j * G + g, R, stride=PITCH), :].astype(jnp.bfloat16)
            both = jnp.concatenate([rows, snap_ref[:, pl.ds(j * 128, 128)]], 0)
            parts.append(jnp.where(live_tile(j % 16, thick, N), both, jnp.zeros((), jnp.bfloat16)))
        stacked = jnp.concatenate(parts, 1)
        gram += lax.dot_general(
            stacked, stacked, (((1,), (1,)), ((), ())), preferred_element_type=jnp.float32
        )
    gram = jnp.concatenate([gram, jnp.zeros((N, 128 - N), jnp.float32)], 1)
    lane = lax.broadcasted_iota(jnp.int32, (16, 128), 1)
    row = lax.broadcasted_iota(jnp.int32, (16, 128), 0)
    thick_block = jnp.where(row * 16 + lane == place, thick.astype(jnp.float32), 0.0)
    upper = jnp.where(lane < 80, gram[0:16], pltpu.roll(gram[32:48], 48, 1))
    last = jnp.where(lane < 112, pltpu.roll(gram[48:64], 32, 1), pltpu.roll(gram[64:80], 48, 1))
    lower = jnp.where(lane < 16, thick_block, jnp.where(lane < 80, gram[16:32], last))
    part_ref[0, 0:16] = upper
    part_ref[0, 16:32] = lower


def gram_partial(thickness, basis, snap):
    return pl.pallas_call(
        gram_body,
        out_shape=pltpu.VMEM((1, 32, 128), jnp.float32),
        in_specs=[smem()] + vmem(2),
        out_specs=vmem()[0],
        scratch_shapes=[pltpu.VMEM((WIDE, 128), jnp.float32), pltpu.VMEM((N, COLS), jnp.bfloat16)],
        compiler_params=pltpu.CompilerParams(vmem_limit_bytes=16 * MIB),
        cost_estimate=pl.CostEstimate(flops=10**9, transcendentals=0, bytes_accessed=10**7),
        name="gram",
    )(thickness, near(basis), near(snap))


def tree_sum(pieces):
    while len(pieces) > 1:
        pieces = [sum(pieces[i + 1 : i + 2], pieces[i]) for i in range(0, len(pieces), 2)]
    return pieces[0]


def combine_body(*refs):
    *ins, out_ref = refs
    pieces = [ref[i] for ref in ins for i in range(ref.shape[0])]
    total = tree_sum(pieces)
    for i in range(out_ref.shape[0]):
        out_ref[i] = total


def combine(arrays, copies):
    return pl.pallas_call(
        combine_body,
        out_shape=pltpu.VMEM((copies, 32, 128), jnp.float32),
        in_specs=vmem(len(arrays)),
        out_specs=vmem()[0],
        compiler_params=pltpu.CompilerParams(vmem_limit_bytes=MIB),
        name="combine",
    )(*(near(a) for a in arrays))


def whole_sum(x):
    return jnp.sum(x, keepdims=True)


def update_body(total_ref, sv_ref, basis_ref, s0, s1, s2, s3, gram_hbm, new_ref, off_hbm, snap_ref, wide_ref, f_ref, out_ref, gram_ref, off_ref, sems):
    g = lax.axis_index("grp")
    core = lax.axis_index("slab_2")
    slab = (lax.axis_index("slab_0") * 4 + lax.axis_index("slab_1")) * 2 + core
    place = g * 64 + slab
    gets = [
        pltpu.make_async_copy(ref, snap_ref.at[g ^ k], sems.at[12 + k])
        for k, ref in enumerate((s0, s1, s2, s3))
    ]
    for get in gets:
        get.start()
    upper, lower = total_ref[0, 0:16], total_ref[0, 16:32]
    lane = lax.broadcasted_iota(jnp.int32, (16, 128), 1)
    row = lax.broadcasted_iota(jnp.int32, (16, 128), 0)
    order = row * 16 + lane
    thick = jnp.where(lane < 16, lower, 0.0)
    off_ref[...] = whole_sum(jnp.where(order < place, thick, 0.0)).astype(jnp.int32)
    put_off = pltpu.make_async_copy(off_ref, off_hbm, sems.at[17])
    put_off.start()
    live = whole_sum(thick) * PLANE
    blocks = (
        upper,
        lower,
        pltpu.roll(upper, 128 - 48, 1),
        pltpu.roll(lower, 128 - 32, 1),
        pltpu.roll(lower, 128 - 48, 1),
    )
    diag = [jnp.where((lane >= 16 * i) & (lane < 80), b, 0.0) for i, b in enumerate(blocks)]
    strict = [jnp.where(lane >= 16 * (i + 1), b, 0.0) for i, b in enumerate(diag)]
    pad = [jnp.zeros((48, 128), jnp.float32)]
    raw = jnp.concatenate(diag + pad, 0) + jnp.concatenate(strict + pad, 0).T
    scale_row = jnp.concatenate([sv_ref[...], jnp.ones((1, 128 - R), jnp.float32)], 1)
    scale_cols = jnp.broadcast_to(scale_row, (128, 128))
    scale_rows = scale_cols.T
    full = raw * scale_rows * scale_cols / (3.0 * live)
    gram_ref[...] = full[:N, :N]
    put_gram = pltpu.make_async_copy(gram_ref, gram_hbm, sems.at[16])
    put_gram.start()
    it = full[:R]
    it = it * (0.5 * R**0.5 / jnp.sqrt(whole_sum(it * it)))
    for i in range(4):
        if i == 3:
            for get in gets:
                get.wait()
        for r in range(i * 16, i * 16 + 16):
            wide_ref[pl.ds(r * PITCH, ROWS), :] = basis_ref[r].astype(jnp.float32)
        prod = lax.dot_general(it, it, (((1,), (1,)), ((), ())), precision=HIGHEST)
        it = 1.5 * it - 0.5 * jnp.dot(prod, it, precision=HIGHEST)
    mix = (it * scale_cols[:R])[:, :N].astype(jnp.bfloat16)
    slab_thick = [
        whole_sum(jnp.where(order == k * 64 + slab, thick, 0.0)) for k in range(G)
    ]
    slab_live = [[jnp.broadcast_to(n, (R, 128)) > p for p in range(4)] for n in slab_thick]
    copies = []

    def compute(lo, hi):
        tiles = range(lo, hi)
        for k in range(G):
            parts = [wide_ref[pl.ds(j * G + k, R, stride=PITCH), :].astype(jnp.bfloat16) for j in tiles]
            snap = snap_ref[k, :, pl.ds(lo * 128, (hi - lo) * 128)]
            stacked = jnp.concatenate([jnp.concatenate(parts, 1), snap], 0)
            res = jnp.dot(mix, stacked, preferred_element_type=jnp.float32)
            for t, j in enumerate(tiles):
                part = jnp.where(slab_live[k][j % 16 // 4], res[:, t * 128 : (t + 1) * 128], 0.0)
                f_ref[pl.ds(j * G + k, R, stride=PITCH), :] = part

    def emit(lo, hi):
        at, rows = lo * G, (hi - lo) * G
        for r in range(R):
            out_ref[r, pl.ds(at, rows), :] = f_ref[pl.ds(r * PITCH + at, rows), :].astype(jnp.bfloat16)
        part = pl.ds(at, rows)
        copy = pltpu.make_async_copy(out_ref.at[:, part], new_ref.at[:, part], sems.at[len(copies)])
        copy.start()
        copies.append(copy)

    compute(0, 4)
    compute(4, 8)
    emit(0, 4)
    compute(8, 12)
    emit(4, 8)
    compute(12, 16)
    emit(8, 12)
    compute(16, 20)
    emit(12, 16)
    compute(20, 24)
    emit(16, 20)
    compute(24, 28)
    emit(20, 24)
    compute(28, 32)
    emit(24, 28)
    compute(32, 36)
    emit(28, 32)
    compute(36, 40)
    emit(32, 36)
    compute(40, 44)
    emit(36, 40)
    compute(44, 48)
    emit(40, 44)
    emit(44, 48)
    for copy in copies + [put_gram, put_off]:
        copy.wait()


def update(total, sv, basis, snaps):
    return pl.pallas_call(
        update_body,
        out_shape=(
            jax.ShapeDtypeStruct((N, N), jnp.float32),
            jax.ShapeDtypeStruct((R, ROWS, 128), jnp.bfloat16),
            jax.ShapeDtypeStruct((1, 1), jnp.int32),
        ),
        in_specs=vmem(3) + hbm(4),
        out_specs=[pl.BlockSpec(memory_space=pl.ANY) for _ in range(3)],
        scratch_shapes=[
            pltpu.VMEM((G, S, COLS), jnp.bfloat16),
            pltpu.VMEM((WIDE, 128), jnp.float32),
            pltpu.VMEM((WIDE, 128), jnp.float32),
            pltpu.VMEM((R, ROWS, 128), jnp.bfloat16),
            pltpu.VMEM((N, N), jnp.float32),
            pltpu.VMEM((1, 1), jnp.int32),
            pltpu.SemaphoreType.DMA((18,)),
        ],
        compiler_params=pltpu.CompilerParams(vmem_limit_bytes=28 * MIB),
        name="update",
    )(near(total), near(sv.reshape(1, R)), near(basis), *(far(s) for s in snaps))


def from_region(snap, k):
    return lax.ppermute(snap, "grp", [(i, i ^ k) for i in range(G)])


def per_device(velocity, old_basis, singular_values, thickness):
    basis = old_basis.reshape(R, 3, G, 16, 128).transpose(0, 1, 3, 2, 4).reshape(R, ROWS, 128)
    snap = snapshots(velocity)
    thickness = lax.optimization_barrier((thickness, snap))[0]
    snaps = [snap] + [from_region(snap, k) for k in (1, 2, 3)]
    part = gram_partial(thickness, basis, snap)
    got = lax.ppermute(part, "slab_2", [(0, 1), (1, 0)])
    spread = combine((part, got), 8)
    got = lax.all_to_all(spread, "slab_0", 0, 0, tiled=True)
    spread = combine((got,), 16)
    got = lax.all_to_all(spread, ("grp", "slab_1"), 0, 0, tiled=True)
    total = combine((got,), 1)
    gram_matrix, new, offsets = update(total, singular_values, basis, snaps)
    new_basis = new.reshape(R, 3, 16, G, 128).transpose(0, 1, 3, 2, 4).reshape(R, 3, G, 2048)
    return (gram_matrix, new_basis, offsets)


def solution(mesh):
    split = Mesh(
        mesh.devices.reshape(mesh.shape["grp"], 8, 4, 2), ("grp", "slab_0", "slab_1", "slab_2")
    )
    in_specs = (P(None, None, "grp", SLAB), P(None, None, None, SLAB), P(), P("grp", SLAB))
    out_specs = (P(), P(None, None, None, SLAB), P("grp", SLAB))
    return jax.shard_map(
        per_device, mesh=split, in_specs=in_specs, out_specs=out_specs, check_vma=False
    )
```
